512 devices in a mesh: attn: 16 (over y, core), expert: 32 (over z, x).
Axes of the slice: x: 4, y: 8, z: 8, core: 2. Of those that a mesh axis runs over, the one named last changes fastest.
Arguments:
- queries: bfloat16 [4096, 4096], P('attn', 'expert'), may hold values from -90 to 90
- keys: bfloat16 [2, 4096, 128], P(None, 'attn'), may hold values from -10 to 10
- values: bfloat16 [2, 4096, 128], P(None, 'attn'), may hold values from -6 to 6
- residual: bfloat16 [4096, 2048], P(('attn', 'expert')), may hold values from -6 to 6
- prompt_lengths: int32 [4], replicated, may hold values from 1 to 3072, 4096 in all
- out_proj: bfloat16 [4096, 2048], P('expert'), may hold values from -0.5 to 0.5
- norm_gain: float32 [2048], replicated, may hold values from 0.1 to 1.9
- expert_ids: int32 [4096, 8], P(('attn', 'expert')), may hold values from 0 to 127, all different within a row; in each aligned block of 8 rows (0 to 7, 8 to 15, ...) at most 2 rows name the same one
- route_weights: float32 [4096, 8], P(('attn', 'expert')), may hold values from 0.02 to 0.4
- w_gate: bfloat16 [32, 2048, 6144], P('expert', None, 'attn'), may hold values from -0.125 to 0.125
- w_up: bfloat16 [32, 2048, 6144], P('expert', None, 'attn'), may hold values from -0.125 to 0.125
- w_down: bfloat16 [32, 6144, 2048], P('expert', 'attn'), may hold values from -0.15625 to 0.15625
Outputs:
- out: bfloat16 [4096, 2048], P(('attn', 'expert'))
The draws below stay inside these ranges and needn't reach their ends.
Inputs may be any that keep to these rules, and one draw needn't show every extreme that they name: `prompt_lengths`: the prompts lie end to end and fill all 4096 positions. `expert_ids`: each row names 8 different experts; within the rows of one device (aligned blocks of 8 rows) no expert is named more than 2 times.
All inputs are finite; a program needn't handle non-finite values.
Results may differ from the reference program's by a relative error of at most 0.015.
Values may be sent and summed in bfloat16 or wider, within the bound.
A program may use at most 64 MiB of HBM per device.

```python
import math
import jax
import jax.numpy as jnp
import numpy as np
from jax import lax

D = 2048
FF = 1536
HEAD_SIZE = 128
KEY_VALUE_HEADS = 2
TOPK = 8
EXP_DEV = 4
PROMPTS = 4
TOK_DEV = 8
QUERY_HEADS = 32
EXPERTS = 128
SEQUENCE_LENGTH = 4096
MOST = 2
HB = 384
SHARDS = 4


def drawn_keys(key):
    return jax.random.truncated_normal(jax.random.fold_in(key, 102), -4.5, 4.5, (KEY_VALUE_HEADS, SEQUENCE_LENGTH, HEAD_SIZE), jnp.float32)


def draw_keys(key, part):
    raw_keys = drawn_keys(key)
    return raw_keys.astype(jnp.bfloat16)


def draw_queries(key, part):
    raw_queries = jax.random.truncated_normal(jax.random.fold_in(key, 104), -4.5, 4.5, (SEQUENCE_LENGTH, QUERY_HEADS * HEAD_SIZE), jnp.float32)
    return raw_queries.astype(jnp.bfloat16)


def shard_levels(stream_key, extent, shards, least, high):
    def one(position, shards_of):
        steps = jax.random.uniform(jax.random.fold_in(jax.random.fold_in(stream_key, 6), position), (shards_of,), jnp.float32, least / len(shards), high / len(shards))
        return jnp.repeat(jnp.exp(steps), extent[position] // shards_of).reshape((-1,) + (1,) * (len(extent) - position - 1))

    gain = one(*shards[0])
    for cut in shards[1:]:
        gain = gain * one(*cut)
    return gain


def split_up(number_of, total, reach, lean):
    loads = [(1 << 20) // math.isqrt(standing ** lean) + 1 for standing in range(2, number_of + 1)]
    rest, given = total - reach - (number_of - 1), [1] * (number_of - 1)
    while rest > 0:
        movable = [i for i in range(number_of - 1) if given[i] < reach]
        whole, remaining = sum([loads[i] for i in movable]), rest
        for i in movable:
            addition = min(reach - given[i], max(1, remaining * loads[i] // whole), rest)
            given[i] = given[i] + addition
            rest = rest - addition
    return np.array([reach] + given)


def ragged_sizes(rng, count, total, bound, skew):
    if count == 2:
        one = jax.random.randint(rng, (), max(1, total - bound), min(bound, total - 1) + 1)
        return jnp.stack([one, total - one])
    tallies = jnp.asarray(split_up(count, total, bound, skew), jnp.int32)
    couples = (count - 1) // 2
    donor, sink = tallies[1:1 + 2 * couples:2], tallies[2:2 + 2 * couples:2]
    slack = jnp.minimum(donor - 1, bound - sink)
    passed = jax.random.randint(jax.random.fold_in(rng, 1), (couples,), 0, 1 << 20) % (slack + 1)
    tallies = tallies.at[1:1 + 2 * couples:2].set(donor - passed).at[2:2 + 2 * couples:2].set(sink + passed)
    return tallies[jax.random.permutation(jax.random.fold_in(rng, 2), count)]


def assign_block(stream_key, own, number, rows, amount, top, reach, lean):
    ranking = jax.random.permutation(stream_key, amount)
    heavy_load, usual = load_shares(amount, rows * top, reach, lean, True), load_shares(amount, rows * top, reach, lean, False)
    places = jnp.arange(amount)

    def named(sizes, offset_by):
        used = int((sizes > 0).sum())
        fixed = max(1, used // 4)
        passed = fixed + (places - fixed + offset_by * (used - fixed)) % max(1, amount - fixed)
        return jnp.zeros((amount,), jnp.int32).at[ranking[jnp.where(places < fixed, places, passed)]].set(jnp.asarray(sizes, jnp.int32))

    sizes = jnp.where(number % 4 == 0, named(heavy_load, number // 4), named(usual, number - number // 4 - 1))
    mixed = jax.random.permutation(jax.random.fold_in(own, 3), amount)
    donor, receiver = mixed[0:amount // 2 * 2:2], mixed[1:amount // 2 * 2:2]
    margin = jnp.minimum(sizes[donor] - 1, reach - sizes[receiver]) // 2
    margin = jnp.where((donor == ranking[0]) | (receiver == ranking[0]) | (sizes[receiver] == 0), 0, jnp.maximum(margin, 0))
    passed = jax.random.randint(jax.random.fold_in(own, 4), (amount // 2,), 0, 1 << 20) % (margin + 1)
    sizes = sizes.at[donor].add(-passed).at[receiver].add(passed)
    members = jnp.searchsorted(jnp.cumsum(sizes), jnp.arange(rows * top), side="right").astype(jnp.int32)
    table = members.reshape(top, rows).T
    table = table[jax.random.permutation(jax.random.fold_in(own, 1), rows)]
    offset_by = jax.random.randint(jax.random.fold_in(own, 2), (rows, 1), 0, top)
    return jnp.take_along_axis(table, (jnp.arange(top)[None, :] + offset_by) % top, axis=1)


def load_shares(count, total, limit, slope, full):
    loads = [(1 << 20) // math.isqrt(grade ** slope) + 1 for grade in range(1, count + 1)]
    largest = limit if full else min(limit, max(-(-total // count), total * loads[0] // sum(loads)))
    least = 1 if total - largest >= count - 1 else 0
    holding, surplus = [largest] + [least] * (count - 1), total - largest - least * (count - 1)
    while surplus > 0:
        free = [i for i in range(1, count) if holding[i] < largest] or [i for i in range(1, count) if holding[i] < limit]
        mass, budget = sum([loads[i] for i in free]), surplus
        for i in free:
            more = min(limit - holding[i], max(1, budget * loads[i] // mass), surplus)
            holding[i] = holding[i] + more
            surplus = surplus - more
    return np.array(holding)


def scatter_about(stream_key, shape, deviation, reach, pieces=(), kind=jnp.bfloat16):
    result = jax.random.normal(stream_key, shape, jnp.float32) * deviation
    if len(pieces) > 0:
        result = shard_levels(stream_key, shape, pieces, -0.22, 0.18) * result
    return jnp.clip(result, min=-reach, max=reach).astype(kind)


def setup_inputs(seed: int = 0) -> dict:
    splits = jax.random.split(jax.random.key(seed), 13)
    queries = draw_queries(jax.random.fold_in(splits[12], 71), 0)
    keys = draw_keys(jax.random.fold_in(splits[12], 71), 0)
    values = scatter_about(splits[2], (KEY_VALUE_HEADS, SEQUENCE_LENGTH, HEAD_SIZE), 1.0, 6.0, ((1, 16),))
    residual = scatter_about(splits[3], (SEQUENCE_LENGTH, D), 1.0, 6.0, ((0, 512),))
    prompt_lengths = ragged_sizes(splits[4], PROMPTS, SEQUENCE_LENGTH, 3 * SEQUENCE_LENGTH // 4, 2).astype(jnp.int32)
    out_proj = scatter_about(splits[5], (QUERY_HEADS * HEAD_SIZE, D), HEAD_SIZE ** -0.5, 0.5, ((0, 32),))
    norm_gain = jnp.clip(1.0 + 0.18 * jax.random.normal(splits[6], (D,), jnp.float32), 0.1, 1.9)
    expert_ids_keys = jax.random.split(jax.random.fold_in(splits[7], 1), SEQUENCE_LENGTH // TOK_DEV)
    expert_ids_turns = jax.random.permutation(jax.random.fold_in(splits[7], 3), SEQUENCE_LENGTH // TOK_DEV)
    expert_ids = jax.vmap(lambda own, number: assign_block(jax.random.fold_in(splits[7], 2), own, number, TOK_DEV, EXPERTS, TOPK, MOST, 2))(expert_ids_keys, expert_ids_turns).reshape((SEQUENCE_LENGTH, TOPK))
    route_weights = jnp.clip(jnp.exp(math.log(0.4) - 2.9957323 * jax.random.uniform(splits[8], (SEQUENCE_LENGTH, TOPK), jnp.float32) ** shard_levels(splits[8], (SEQUENCE_LENGTH, TOPK), ((0, 512),), -0.2, 0.2)), 0.02, 0.4)
    w_gate = scatter_about(splits[9], (EXPERTS // EXP_DEV, D, EXP_DEV * FF), D ** -0.5, 0.125, ((0, 32), (2, 16)))
    w_up = scatter_about(splits[10], (EXPERTS // EXP_DEV, D, EXP_DEV * FF), D ** -0.5, 0.125, ((0, 32), (2, 16)))
    w_down = scatter_about(splits[11], (EXPERTS // EXP_DEV, EXP_DEV * FF, D), FF ** -0.5, 0.15625, ((0, 32), (1, 16)))
    return {"queries": queries, "keys": keys, "values": values, "residual": residual, "prompt_lengths": prompt_lengths, "out_proj": out_proj, "norm_gain": norm_gain, "expert_ids": expert_ids, "route_weights": route_weights, "w_gate": w_gate, "w_up": w_up, "w_down": w_down}


def prompt_owner(places, prompt_lengths):
    prompt_ends = jnp.cumsum(prompt_lengths)
    return lax.optimization_barrier(jnp.sum((places[:, None] >= prompt_ends[None, :-1]).astype(jnp.int32), axis=1))

def reference(queries, keys, values, residual, prompt_lengths, out_proj, norm_gain, expert_ids, route_weights, w_gate, w_up, w_down):
    score_scale = 1.0 / math.sqrt(HEAD_SIZE)
    block_rows = math.gcd(SEQUENCE_LENGTH, 512)
    query_group_count = QUERY_HEADS // KEY_VALUE_HEADS
    places = jnp.arange(SEQUENCE_LENGTH, dtype=jnp.int32)
    owners = prompt_owner(places, prompt_lengths)

    def one_head(head_index):
        head_queries = lax.dynamic_slice_in_dim(queries, head_index * HEAD_SIZE, HEAD_SIZE, 1)
        head_keys = lax.dynamic_index_in_dim(keys, head_index // query_group_count, 0, keepdims=False)
        head_values = lax.dynamic_index_in_dim(values, head_index // query_group_count, 0, keepdims=False)

        def one_block(offset):
            block_queries = lax.dynamic_slice_in_dim(head_queries, offset, block_rows, 0)
            query_places = offset + jnp.arange(block_rows, dtype=jnp.int32)
            query_owner = lax.dynamic_slice_in_dim(owners, offset, block_rows, 0)
            visible = (places[None, :] <= query_places[:, None]) & (owners[None, :] == query_owner[:, None])
            scores = lax.dot_general(block_queries, head_keys, (((1,), (1,)), ((), ())), preferred_element_type=jnp.float32) * score_scale
            scores = jnp.where(visible, scores, -1e+30)
            highest = lax.optimization_barrier(jnp.max(scores, axis=1, keepdims=True))
            weights = jnp.where(visible, jnp.exp(scores - highest), 0.0)
            weight_sum = lax.optimization_barrier(jnp.sum(weights, axis=1, keepdims=True))
            weighted = jnp.dot(weights.astype(jnp.bfloat16), head_values, preferred_element_type=jnp.float32)
            return (weighted / weight_sum).astype(jnp.bfloat16)
        offsets = jnp.arange(SEQUENCE_LENGTH // block_rows, dtype=jnp.int32) * block_rows
        return lax.map(one_block, offsets).reshape(SEQUENCE_LENGTH, HEAD_SIZE)
    attended = lax.map(one_head, jnp.arange(QUERY_HEADS, dtype=jnp.int32))

    def add_head(carried, head_index):
        head_rows = lax.dynamic_slice_in_dim(out_proj, head_index * HEAD_SIZE, HEAD_SIZE, 0)
        head_term = jnp.dot(attended[head_index], head_rows, preferred_element_type=jnp.float32)
        head_term = lax.optimization_barrier(head_term.astype(jnp.bfloat16)).astype(jnp.float32)
        return (carried + head_term, None)
    projected = lax.scan(add_head, jnp.zeros((SEQUENCE_LENGTH, D), jnp.float32), jnp.arange(QUERY_HEADS, dtype=jnp.int32))[0]
    stream = residual.astype(jnp.float32) + projected
    mean_square = lax.optimization_barrier(jnp.mean(stream * stream, axis=1, keepdims=True))
    normalized = (stream * lax.rsqrt(mean_square + 1e-06) * norm_gain).astype(jnp.bfloat16)
    block_count = SEQUENCE_LENGTH // TOK_DEV
    inside = jnp.arange(TOK_DEV, dtype=jnp.int32)
    block_starts = jnp.arange(block_count, dtype=jnp.int32) * TOK_DEV

    def one_expert(carried, expert):
        matches = expert_ids == expert
        weight_sum = lax.optimization_barrier(jnp.sum(jnp.where(matches, route_weights, 0.0), axis=1))
        routed = jnp.any(matches, axis=1).reshape(block_count, TOK_DEV)
        ranked = jnp.cumsum(routed.astype(jnp.int32), axis=1) - 1
        chosen_rows = []
        filled_slots = []
        for slot_index in range(MOST):
            chosen = routed & (ranked == slot_index)
            filled_slots.append(jnp.any(chosen, axis=1))
            chosen_rows.append(block_starts + lax.optimization_barrier(jnp.sum(jnp.where(chosen, inside[None, :], 0), axis=1)).astype(jnp.int32))
        token_rows = jnp.stack(chosen_rows, axis=1).reshape(-1)
        filled = jnp.stack(filled_slots, axis=1).reshape(-1)
        inputs = normalized[token_rows]
        column = expert // EXP_DEV
        within = expert % EXP_DEV
        gate_cols = lax.dynamic_slice_in_dim(lax.dynamic_index_in_dim(w_gate, column, 0, keepdims=False), within * FF, FF, 1)
        up_cols = lax.dynamic_slice_in_dim(lax.dynamic_index_in_dim(w_up, column, 0, keepdims=False), within * FF, FF, 1)
        down_rows = lax.dynamic_slice_in_dim(lax.dynamic_index_in_dim(w_down, column, 0, keepdims=False), within * FF, FF, 0)
        gate_part = jnp.dot(inputs, gate_cols, preferred_element_type=jnp.float32)
        up_part = jnp.dot(inputs, up_cols, preferred_element_type=jnp.float32)
        active = (jax.nn.silu(gate_part) * up_part).astype(jnp.bfloat16)
        expert_out = jnp.zeros((token_rows.shape[0], D), jnp.float32)
        for shard_index in range(SHARDS):
            piece_out = jnp.dot(active[:, shard_index * HB:(shard_index + 1) * HB], down_rows[shard_index * HB:(shard_index + 1) * HB], preferred_element_type=jnp.float32)
            expert_out = expert_out + lax.optimization_barrier(piece_out.astype(jnp.bfloat16)).astype(jnp.float32)
        scaled = expert_out * (weight_sum[token_rows] * filled.astype(jnp.float32))[:, None]
        return (carried.at[token_rows].add(scaled), None)
    mixed = lax.scan(one_expert, jnp.zeros((SEQUENCE_LENGTH, D), jnp.float32), jnp.arange(EXPERTS, dtype=jnp.int32))[0]
    return (stream + mixed).astype(jnp.bfloat16)
```

```python
import functools
import math

import jax
import jax.numpy as jnp
from jax import lax
from jax.experimental import pallas as pl
from jax.experimental.pallas import tpu as pltpu
from jax.sharding import PartitionSpec as P

BF = jnp.bfloat16
F32 = jnp.float32
VM = pltpu.VMEM
DMA = pltpu.SemaphoreType.DMA
D = 2048
DM = D + 128
RING = 8
XS = 4
QSCALE = math.log2(math.e) / math.sqrt(128.0)
ORDER = (4, 3, 5, 2, 6, 1, 7, 0)
SLOTS = (0, 1, 7, 2, 6, 3, 5, 4)


def remote(src, dst, send, recv, **dev):
    return pltpu.make_async_remote_copy(
        src_ref=src,
        dst_ref=dst,
        send_sem=send,
        recv_sem=recv,
        device_id=dev,
        device_id_type=pl.DeviceIdType.MESH,
    )


def greet(peers):
    barrier = pltpu.get_barrier_semaphore()
    for peer in peers:
        pl.semaphore_signal(barrier, inc=1, device_id=peer, device_id_type=pl.DeviceIdType.MESH)
    pl.semaphore_wait(barrier, len(peers))


def attention_kernel(
    lengths, q_ref, k_ref, v_ref, wo_ref, wg_ref, wu_ref, wd_ref,
    out_ref, pg_ref, pu_ref, pd_ref,
    kbuf, vbuf, m_ref, l_ref, acc_ref, send, recv, wsend, wrecv,
):
    a = lax.axis_index("attn")
    e = lax.axis_index("expert")
    y = a // 2
    c = a % 2
    head = e // 16
    right = ((y + 1) % RING) * 2 + c
    left = ((y + RING - 1) % RING) * 2 + c
    partner = y * 2 + (1 - c)
    greet([{"attn": right}, {"attn": left}, {"attn": partner}])
    bufs = (kbuf, vbuf)
    ins = (k_ref, v_ref)
    pending = []

    def push(kv, src, block, slot, way):
        to = (right, left, partner)[way]
        copy = remote(
            src, bufs[kv].at[block], send.at[kv, slot, way], recv.at[kv, block], attn=to
        )
        copy.start()
        pending.append(copy)

    def arrived(kv, block):
        remote(
            bufs[kv].at[block], bufs[kv].at[block], send.at[kv, 0, 0], recv.at[kv, block],
            attn=partner,
        ).wait_recv()

    wcopies = []

    def swap(step):
        for n, (mine, theirs, rows) in enumerate(
            ((wg_ref, pg_ref, 512), (wu_ref, pu_ref, 512), (wd_ref, pd_ref, 96))
        ):
            part = pl.ds(step * rows, rows)
            copy = remote(
                mine.at[0, part], theirs.at[part], wsend.at[n, step], wrecv.at[n, step],
                attn=partner,
            )
            copy.start()
            wcopies.append(copy)

    for way in (2, 0, 1):
        for kv in range(2):
            push(kv, ins[kv].at[head], a, 0, way)
    swap(0)
    kbuf[pl.ds(a, 1)] = k_ref[pl.ds(head, 1)]
    vbuf[pl.ds(a, 1)] = v_ref[pl.ds(head, 1)]

    end1 = lengths[0]
    end2 = end1 + lengths[1]
    end3 = end2 + lengths[2]
    qpos = a * 256 + lax.broadcasted_iota(jnp.int32, (256, 1), 0)
    first = jnp.where(
        qpos >= end3, end3, jnp.where(qpos >= end2, end2, jnp.where(qpos >= end1, end1, 0))
    )
    m_ref[...] = jnp.full((256, 1), -1e30, F32)
    l_ref[...] = jnp.zeros((256, 1), F32)
    acc_ref[...] = jnp.zeros((256, 128), F32)

    def attend(chunk):
        kc = kbuf[pl.ds(chunk * 2, 2)].reshape(512, 128)
        vc = vbuf[pl.ds(chunk * 2, 2)].reshape(512, 128)
        scores = lax.dot_general(
            q_ref[...], kc, (((1,), (1,)), ((), ())), preferred_element_type=F32
        )
        kpos = chunk * 512 + lax.broadcasted_iota(jnp.int32, (256, 512), 1)
        scores = jnp.where((kpos >= first) & (kpos <= qpos), scores * QSCALE, -1e30)
        old = m_ref[...]
        new = jnp.maximum(old, jnp.max(scores, axis=1, keepdims=True))
        factor = jnp.exp2(old - new)
        weights = jnp.exp2(scores - new)
        m_ref[...] = new
        l_ref[...] = l_ref[...] * factor + jnp.sum(weights, axis=1, keepdims=True)
        acc_ref[...] = acc_ref[...] * factor + jnp.dot(
            weights.astype(BF), vc, preferred_element_type=F32
        )

    for kv in range(2):
        arrived(kv, partner)
    attend(y)
    for step in range(1, 5):
        below = (y + RING - step) % RING
        above = (y + step) % RING
        if step < 4:
            for kv in range(2):
                arrived(kv, below * 2 + c)
                if step < 3 or kv == 0:
                    push(kv, bufs[kv].at[below * 2 + c], below * 2 + c, step, 0)
                push(kv, bufs[kv].at[below * 2 + c], below * 2 + c, step, 2)
            for kv in range(2):
                arrived(kv, above * 2 + c)
                if step < 3 or kv == 1:
                    push(kv, bufs[kv].at[above * 2 + c], above * 2 + c, RING - step, 1)
                push(kv, bufs[kv].at[above * 2 + c], above * 2 + c, RING - step, 2)
            swap(step)
        else:
            for kv in range(2):
                arrived(kv, below * 2 + c)
                push(kv, bufs[kv].at[below * 2 + c], below * 2 + c, 4, 2)
        for chunk in (below, above) if step < 4 else (below,):
            for kv in range(2):
                arrived(kv, chunk * 2 + (1 - c))

            @pl.when(chunk <= y)
            def _():
                attend(chunk)

    attended = (acc_ref[...] / l_ref[...]).astype(BF)
    for n in range(4):
        cols = slice(n * 512, (n + 1) * 512)
        term = jnp.dot(attended, wo_ref[:, cols], preferred_element_type=F32)
        out_ref[:, cols] = term.astype(BF)
    for copy in pending:
        copy.wait_send()
    for copy in wcopies:
        copy.wait()


def mix_heads_kernel(
    ht_ref, res_ref, gain_ref, meta_ref, stream_ref, gy_ref,
    via, fromleft, fromright, fwd, part, zin, nbuf, gbuf,
    s1, s2, s3, rvia, rleft, rright, rz, sy, ry,
):
    a = lax.axis_index("attn")
    e = lax.axis_index("expert")
    y = a // 2
    c = a % 2
    z = e // XS
    x = e % XS
    xr = (x + 1) % XS
    xl = (x + 3) % XS
    xo = (x + 2) % XS
    right = z * XS + xr
    left = z * XS + xl
    zs = [((z + r) % RING) for r in range(RING)]
    peers = [{"expert": right}, {"expert": left}]
    peers += [{"expert": zs[r] * XS + x} for r in range(1, RING)]
    ys = [((y + r) % RING) for r in range(RING)]
    peers += [{"attn": ys[r] * 2 + c} for r in range(1, RING)]
    greet(peers)
    pending = []

    def push(*args, **dev):
        copy = remote(*args, **dev)
        copy.start()
        pending.append(copy)

    def got(buf, sem):
        remote(buf, buf, sem, sem, expert=left).wait_recv()

    def block(r, col):
        return ht_ref.at[zs[r], col]

    for n, r in enumerate(ORDER):
        if n % 2 == 0:
            push(block(r, xo), via.at[r], s1.at[r, 0], rvia.at[r], expert=right)
            push(block(r, xl), fromright.at[r], s1.at[r, 1], rright.at[r], expert=left)
        else:
            push(block(r, xo), via.at[r], s1.at[r, 0], rvia.at[r], expert=left)
            push(block(r, xr), fromleft.at[r], s1.at[r, 1], rleft.at[r], expert=right)
    total = res_ref[...].astype(F32)
    for n in range(RING + 2):
        if n < RING:
            r = ORDER[n]
            got(via.at[r], rvia.at[r])
            col = xr if n % 2 == 0 else xl
            mine = ht_ref[pl.ds(zs[r], 1), pl.ds(col, 1)].reshape(8, D).astype(F32)
            fwd[r] = (via[r].astype(F32) + mine).astype(BF)
            if n % 2 == 0:
                push(fwd.at[r], fromleft.at[r], s2.at[r], rleft.at[r], expert=right)
            else:
                push(fwd.at[r], fromright.at[r], s2.at[r], rright.at[r], expert=left)
        if n >= 2:
            r = ORDER[n - 2]
            got(fromleft.at[r], rleft.at[r])
            got(fromright.at[r], rright.at[r])
            mine = ht_ref[pl.ds(zs[r], 1), pl.ds(x, 1)].reshape(8, D).astype(F32)
            summed = mine + fromleft[r].astype(F32) + fromright[r].astype(F32)
            if r == 0:
                total = total + summed
            else:
                part[r] = summed.astype(BF)
                push(part.at[r], zin.at[r], s3.at[r], rz.at[r], expert=zs[r] * XS + x)
    for r in ORDER[:-1]:
        got(zin.at[r], rz.at[r])
        total = total + zin[r].astype(F32)
    stream_ref[...] = total
    mean = jnp.mean(total * total, axis=1, keepdims=True)
    nbuf[:, :D] = (total * lax.rsqrt(mean + 1e-06) * gain_ref[...]).astype(BF)
    nbuf[:, D:] = meta_ref[...]
    gbuf[pl.ds(y, 1)] = nbuf[...].reshape(1, 8, DM)
    for r in ORDER[:-1]:
        push(nbuf, gbuf.at[y], sy.at[r], ry.at[r], attn=ys[r] * 2 + c)
    for r in range(1, RING):
        src = (y + RING - r) % RING
        got(gbuf.at[src], ry.at[r])
    for n in range(4):
        pair = gbuf[2 * n : 2 * n + 2].astype(F32).reshape(16, DM)
        gy_ref[16 * n : 16 * n + 16, :] = pair.astype(BF)
    for copy in pending:
        copy.wait_send()


def experts_kernel(
    gy_ref, stream_ref, wg_ref, wu_ref, wd_ref, pg_ref, pu_ref, pd_ref,
    out_ref,
    wg, wu, wd, toks, chosen, rows, dvia, act, outs, back, bvia, chi, clo,
    zsum, zgot, zlast, ysum, ygot,
    wsem, tsend, trecv, dsend, drecv, dvs, dvr, bsend, brecv, bvs, bvr,
    zsend, zrecv, zfin, ysend, yrecv,
):
    a = lax.axis_index("attn")
    e = lax.axis_index("expert")
    y = a // 2
    c = a % 2
    quarter = a // 4
    z = e // XS
    x = e % XS
    xr = (x + 1) % XS
    xl = (x + 3) % XS
    xo = (x + 2) % XS
    right = z * XS + xr
    left = z * XS + xl
    up = ((z + 1) % RING) * XS + x
    down = ((z + RING - 1) % RING) * XS + x
    ys = [((y + r) % RING) for r in range(RING)]
    loads = []
    for n, (src, dst) in enumerate(
        (
            (wg_ref.at[0], wg.at[:, 0:384]),
            (pg_ref, wg.at[:, 384:768]),
            (wu_ref.at[0], wu.at[:, 0:384]),
            (pu_ref, wu.at[:, 384:768]),
            (wd_ref.at[0], wd.at[0:384]),
            (pd_ref, wd.at[384:768]),
        )
    ):
        load = pltpu.make_async_copy(src, dst, wsem.at[n])
        load.start()
        loads.append(load)
    peers = [{"expert": right}, {"expert": left}, {"expert": up}, {"expert": down}]
    peers += [{"attn": ys[r] * 2 + c} for r in range(1, RING)]
    greet(peers)
    pending = []

    def push(*args, **dev):
        copy = remote(*args, **dev)
        copy.start()
        pending.append(copy)

    def got(buf, sem):
        remote(buf, buf, sem, sem, expert=left).wait_recv()

    def half(ref, slot, h):
        return ref.at[slot, pl.ds(32 * h, 32)]

    for h in range(2):
        own = gy_ref.at[pl.ds(32 * h, 32)]
        push(own, half(toks, 1, h), tsend.at[0, h, 0], trecv.at[1, h], expert=up)
        push(own, half(toks, 7, h), tsend.at[0, h, 1], trecv.at[7, h], expert=down)
    toks[0] = gy_ref[...]

    tok = lax.broadcasted_iota(jnp.int32, (64, 64), 0)
    col = lax.broadcasted_iota(jnp.int32, (64, 64), 1)
    earlier = ((tok // 8 == col // 8) & (col < tok)).astype(F32).astype(BF)
    lane = lax.broadcasted_iota(jnp.int32, (64, 128), 1)

    def choose(s):
        meta = toks[s, :, D:DM].astype(F32)
        high = pltpu.roll(meta, 120, 1)
        low = pltpu.roll(meta, 112, 1)
        hit = jnp.zeros((64, 64), F32)
        whi = jnp.zeros((64, 64), F32)
        wlo = jnp.zeros((64, 64), F32)
        for k in range(XS):
            expert = (4 * (z * XS + k) + quarter).astype(F32)
            match = (meta == expert) & (lane < 8)
            here = col // 16 == k
            hit = jnp.where(here, jnp.sum(jnp.where(match, 1.0, 0.0), 1, keepdims=True), hit)
            whi = jnp.where(here, jnp.sum(jnp.where(match, high, 0.0), 1, keepdims=True), whi)
            wlo = jnp.where(here, jnp.sum(jnp.where(match, low, 0.0), 1, keepdims=True), wlo)
        before = jnp.dot(earlier, hit.astype(BF), preferred_element_type=F32)
        place = (2 * (tok // 8)).astype(F32) + before
        pick = jnp.where((col % 16).astype(F32) == place, hit, 0.0)
        chi[s] = (pick * whi).astype(BF)
        clo[s] = (pick * wlo).astype(BF)
        pick = pick.astype(BF)
        for n in range(4):
            cols = slice(n * 512, (n + 1) * 512)
            got_rows = lax.dot_general(
                pick, toks[s, :, cols], (((0,), (0,)), ((), ())), preferred_element_type=F32
            )
            chosen[s, :, :, cols] = got_rows.astype(BF).reshape(XS, 16, 512)

    def ffn(s):
        block = rows[s].reshape(64, D)
        for n in range(3):
            cols = slice(n * 256, (n + 1) * 256)
            gate = jnp.dot(block, wg[:, cols], preferred_element_type=F32)
            lift = jnp.dot(block, wu[:, cols], preferred_element_type=F32)
            act[:, cols] = (gate / (1.0 + jnp.exp(-gate)) * lift).astype(BF)
        for n in range(4):
            cols = slice(n * 512, (n + 1) * 512)
            made = jnp.dot(act[...], wd[:, cols], preferred_element_type=F32)
            outs[s, :, :, cols] = made.astype(BF).reshape(XS, 16, 512)

    def spread(s, src, dst, via, ss, rr, vr):
        push(src.at[s, xr], dst.at[s, x], ss.at[s, 0], rr.at[s, x], expert=right)
        push(src.at[s, xl], dst.at[s, x], ss.at[s, 1], rr.at[s, x], expert=left)
        push(
            src.at[s, xo], via.at[s], ss.at[s, 2], vr.at[s],
            expert=right if SLOTS.index(s) % 2 == 0 else left,
        )

    def relay(s, dst, via, vs, rr, vr):
        got(via.at[s], vr.at[s])
        if SLOTS.index(s) % 2 == 0:
            push(via.at[s], dst.at[s, xl], vs.at[s], rr.at[s, xl], expert=right)
        else:
            push(via.at[s], dst.at[s, xr], vs.at[s], rr.at[s, xr], expert=left)

    for n in range(RING + 3):
        if n < RING:
            s = SLOTS[n]
            if s:
                for h in range(2):
                    got(half(toks, s, h), trecv.at[s, h])
                    if s < 3 or (s == 3 and h == 0):
                        push(
                            half(toks, s, h), half(toks, s + 1, h), tsend.at[s, h, 0],
                            trecv.at[s + 1, h], expert=up,
                        )
                    if s > 5 or (s == 5 and h == 1):
                        push(
                            half(toks, s, h), half(toks, s - 1, h), tsend.at[s, h, 1],
                            trecv.at[s - 1, h], expert=down,
                        )
            choose(s)
            spread(s, chosen, rows, dvia, dsend, drecv, dvr)
            rows[s, pl.ds(x, 1)] = chosen[s, pl.ds(x, 1)]
        if 1 <= n < RING + 1:
            relay(SLOTS[n - 1], rows, dvia, dvs, drecv, dvr)
        if 2 <= n < RING + 2:
            s = SLOTS[n - 2]
            for k in (xl, xr, xo):
                got(rows.at[s, k], drecv.at[s, k])
            if n == 2:
                for load in loads:
                    load.wait()
            ffn(s)
            spread(s, outs, back, bvia, bsend, brecv, bvr)
            back[s, pl.ds(x, 1)] = outs[s, pl.ds(x, 1)]
        if 3 <= n:
            relay(SLOTS[n - 3], back, bvia, bvs, brecv, bvr)

    def combine(s, h):
        part = slice(32 * h, 32 * h + 32)
        made = back[s].reshape(64, D)
        return jnp.dot(chi[s, part, :], made, preferred_element_type=F32) + jnp.dot(
            clo[s, part, :], made, preferred_element_type=F32
        )

    for s in reversed(SLOTS):
        for k in (xl, xr, xo):
            got(back.at[s, k], brecv.at[s, k])
        for h in range(2):
            value = combine(s, h)
            part = slice(32 * h, 32 * h + 32)
            if s == 0:
                for way in range(2):
                    got(zlast.at[way, pl.ds(32 * h, 32)], zfin.at[way, h])
                    value = value + zlast[way, part, :].astype(F32)
                for j in range(4):
                    row = 4 * h + j
                    ysum[row] = value[8 * j : 8 * j + 8].astype(BF)
                continue
            if s in (1, 2, 6, 7) or (s == 3 and h == 0) or (s == 5 and h == 1):
                got(half(zgot, s, h), zrecv.at[s, h])
                value = value + zgot[s, part, :].astype(F32)
            zsum[s, part, :] = value.astype(BF)
            downward = s < 4 or (s == 4 and h == 0)
            to = s - 1 if downward else (s + 1) % RING
            if to == 0:
                way = 0 if downward else 1
                push(
                    half(zsum, s, h), zlast.at[way, pl.ds(32 * h, 32)], zsend.at[s, h],
                    zfin.at[way, h], expert=down if downward else up,
                )
            else:
                push(
                    half(zsum, s, h), half(zgot, to, h), zsend.at[s, h], zrecv.at[to, h],
                    expert=down if downward else up,
                )
    for r in ORDER[:-1]:
        push(ysum.at[ys[r]], ygot.at[r], ysend.at[r], yrecv.at[r], attn=ys[r] * 2 + c)
    total = stream_ref[...] + ysum[pl.ds(y, 1)].reshape(8, D).astype(F32)
    for r in range(1, RING):
        got(ygot.at[r], yrecv.at[r])
        total = total + ygot[r].astype(F32)
    out_ref[...] = total.astype(BF)
    for copy in pending:
        copy.wait_send()


def vmem(*shape, dtype=BF):
    return VM(shape, dtype)


def local(
    queries, keys, values, residual, prompt_lengths, out_proj, norm_gain,
    expert_ids, route_weights, w_gate, w_up, w_down,
):
    inv = pl.BlockSpec(memory_space=VM)
    anyw = pl.BlockSpec(memory_space=pl.ANY)
    smem = pl.BlockSpec(memory_space=pltpu.SMEM)
    high = lax.reduce_precision(route_weights, 8, 7)
    low = route_weights - high
    meta = jnp.concatenate(
        [expert_ids.astype(F32), high, low, jnp.zeros((8, 104), F32)], axis=1
    ).astype(BF)

    terms, pg, pu, pd = pl.pallas_call(
        attention_kernel,
        out_shape=(
            jax.ShapeDtypeStruct((256, D), BF),
            jax.ShapeDtypeStruct((D, 384), BF),
            jax.ShapeDtypeStruct((D, 384), BF),
            jax.ShapeDtypeStruct((384, D), BF),
        ),
        in_specs=[smem, inv, inv, inv, inv, anyw, anyw, anyw],
        out_specs=(inv, anyw, anyw, anyw),
        scratch_shapes=[
            vmem(16, 256, 128),
            vmem(16, 256, 128),
            vmem(256, 1, dtype=F32),
            vmem(256, 1, dtype=F32),
            vmem(256, 128, dtype=F32),
            DMA((2, 8, 3)),
            DMA((2, 16)),
            DMA((3, 4)),
            DMA((3, 4)),
        ],
        compiler_params=pltpu.CompilerParams(collective_id=0, has_side_effects=True),
        name="attention",
    )(prompt_lengths, queries, keys, values, out_proj, w_gate, w_up, w_down)

    stream, rows = pl.pallas_call(
        mix_heads_kernel,
        out_shape=(jax.ShapeDtypeStruct((8, D), F32), jax.ShapeDtypeStruct((64, DM), BF)),
        in_specs=[inv] * 4,
        out_specs=(inv, inv),
        scratch_shapes=[vmem(8, 8, D)] * 6
        + [vmem(8, DM), vmem(8, 8, DM)]
        + [DMA((8, 2))]
        + [DMA((8,))] * 8,
        compiler_params=pltpu.CompilerParams(collective_id=1, has_side_effects=True),
        name="mix_heads",
    )(terms.reshape(8, 4, 8, D), residual, norm_gain.reshape(1, D), meta)

    return pl.pallas_call(
        experts_kernel,
        out_shape=jax.ShapeDtypeStruct((8, D), BF),
        in_specs=[inv, inv] + [anyw] * 6,
        out_specs=inv,
        scratch_shapes=[
            vmem(D, 768),
            vmem(D, 768),
            vmem(768, D),
            vmem(8, 64, DM),
            vmem(8, 4, 16, D),
            vmem(8, 4, 16, D),
            vmem(8, 16, D),
            vmem(64, 768),
            vmem(8, 4, 16, D),
            vmem(8, 4, 16, D),
            vmem(8, 16, D),
            vmem(8, 64, 64),
            vmem(8, 64, 64),
            vmem(8, 64, D),
            vmem(8, 64, D),
            vmem(2, 64, D),
            vmem(8, 8, D),
            vmem(8, 8, D),
            DMA((6,)),
            DMA((8, 2, 2)),
            DMA((8, 2)),
            DMA((8, 3)),
            DMA((8, 4)),
            DMA((8,)),
            DMA((8,)),
            DMA((8, 3)),
            DMA((8, 4)),
            DMA((8,)),
            DMA((8,)),
            DMA((8, 2)),
            DMA((8, 2)),
            DMA((2, 2)),
            DMA((8,)),
            DMA((8,)),
        ],
        compiler_params=pltpu.CompilerParams(collective_id=2, has_side_effects=True),
        name="experts",
    )(rows, stream, w_gate, w_up, w_down, pg, pu, pd)


def solution(mesh):
    return jax.shard_map(
        local,
        mesh=mesh,
        in_specs=(
            P("attn", "expert"),
            P(None, "attn", None),
            P(None, "attn", None),
            P(("attn", "expert"), None),
            P(),
            P("expert", None),
            P(),
            P(("attn", "expert"), None),
            P(("attn", "expert"), None),
            P("expert", None, "attn"),
            P("expert", None, "attn"),
            P("expert", "attn", None),
        ),
        out_specs=P(("attn", "expert"), None),
        check_vma=False,
    )
```

```python
import math

import jax
import jax.numpy as jnp
from jax import lax
from jax.experimental import pallas as pl
from jax.experimental.pallas import tpu as pltpu
from jax.sharding import PartitionSpec as P

BF = jnp.bfloat16
F32 = jnp.float32
VM = pltpu.VMEM
DMA = pltpu.SemaphoreType.DMA
D = 2048
EX = 640
W = D - EX
TW = W + 128
CUTS = ((0, 512), (512, 1024), (1024, W))
RING = 8
XS = 4
QSCALE = math.log2(math.e) / math.sqrt(128.0)
ORDER = (4, 3, 5, 2, 6, 1, 7, 0)
SLOTS = (0, 1, 7, 2, 6, 3, 5, 4)


def remote(src, dst, send, recv, **dev):
    return pltpu.make_async_remote_copy(
        src_ref=src,
        dst_ref=dst,
        send_sem=send,
        recv_sem=recv,
        device_id=dev,
        device_id_type=pl.DeviceIdType.MESH,
    )


def greet(peers):
    barrier = pltpu.get_barrier_semaphore()
    for peer in peers:
        pl.semaphore_signal(barrier, inc=1, device_id=peer, device_id_type=pl.DeviceIdType.MESH)
    pl.semaphore_wait(barrier, len(peers))


def attention_kernel(
    lengths, q_ref, k_ref, v_ref, wo_ref, wg_ref, wu_ref, wd_ref,
    out_ref, pg_ref, pu_ref, pd_ref,
    kbuf, vbuf, m_ref, l_ref, acc_ref, send, recv, wsend, wrecv,
):
    a = lax.axis_index("attn")
    e = lax.axis_index("expert")
    y = a // 2
    c = a % 2
    head = e // 16
    right = ((y + 1) % RING) * 2 + c
    left = ((y + RING - 1) % RING) * 2 + c
    partner = y * 2 + (1 - c)
    greet([{"attn": right}, {"attn": left}, {"attn": partner}])
    bufs = (kbuf, vbuf)
    ins = (k_ref, v_ref)
    pending = []

    def push(kv, src, block, slot, way):
        to = (right, left, partner)[way]
        copy = remote(
            src, bufs[kv].at[block], send.at[kv, slot, way], recv.at[kv, block], attn=to
        )
        copy.start()
        pending.append(copy)

    def arrived(kv, block):
        remote(
            bufs[kv].at[block], bufs[kv].at[block], send.at[kv, 0, 0], recv.at[kv, block],
            attn=partner,
        ).wait_recv()

    wcopies = []

    def swap(step):
        for n, (mine, theirs, rows) in enumerate(
            ((wg_ref, pg_ref, 512), (wu_ref, pu_ref, 512), (wd_ref, pd_ref, 96))
        ):
            part = pl.ds(step * rows, rows)
            copy = remote(
                mine.at[0, part], theirs.at[part], wsend.at[n, step], wrecv.at[n, step],
                attn=partner,
            )
            copy.start()
            wcopies.append(copy)

    for way in (2, 0, 1):
        for kv in range(2):
            push(kv, ins[kv].at[head], a, 0, way)
    swap(0)
    kbuf[pl.ds(a, 1)] = k_ref[pl.ds(head, 1)]
    vbuf[pl.ds(a, 1)] = v_ref[pl.ds(head, 1)]

    end1 = lengths[0]
    end2 = end1 + lengths[1]
    end3 = end2 + lengths[2]
    qpos = a * 256 + lax.broadcasted_iota(jnp.int32, (256, 1), 0)
    first = jnp.where(
        qpos >= end3, end3, jnp.where(qpos >= end2, end2, jnp.where(qpos >= end1, end1, 0))
    )
    m_ref[...] = jnp.full((256, 1), -1e30, F32)
    l_ref[...] = jnp.zeros((256, 1), F32)
    acc_ref[...] = jnp.zeros((256, 128), F32)

    def attend(chunk):
        kc = kbuf[pl.ds(chunk * 2, 2)].reshape(512, 128)
        vc = vbuf[pl.ds(chunk * 2, 2)].reshape(512, 128)
        scores = lax.dot_general(
            q_ref[...], kc, (((1,), (1,)), ((), ())), preferred_element_type=F32
        )
        kpos = chunk * 512 + lax.broadcasted_iota(jnp.int32, (256, 512), 1)
        scores = jnp.where((kpos >= first) & (kpos <= qpos), scores * QSCALE, -1e30)
        old = m_ref[...]
        new = jnp.maximum(old, jnp.max(scores, axis=1, keepdims=True))
        factor = jnp.exp2(old - new)
        weights = jnp.exp2(scores - new)
        m_ref[...] = new
        l_ref[...] = l_ref[...] * factor + jnp.sum(weights, axis=1, keepdims=True)
        acc_ref[...] = acc_ref[...] * factor + jnp.dot(
            weights.astype(BF), vc, preferred_element_type=F32
        )

    for kv in range(2):
        arrived(kv, partner)
    attend(y)
    for step in range(1, 5):
        below = (y + RING - step) % RING
        above = (y + step) % RING
        if step < 4:
            for kv in range(2):
                arrived(kv, below * 2 + c)
                if step < 3 or kv == 0:
                    push(kv, bufs[kv].at[below * 2 + c], below * 2 + c, step, 0)
                push(kv, bufs[kv].at[below * 2 + c], below * 2 + c, step, 2)
            for kv in range(2):
                arrived(kv, above * 2 + c)
                if step < 3 or kv == 1:
                    push(kv, bufs[kv].at[above * 2 + c], above * 2 + c, RING - step, 1)
                push(kv, bufs[kv].at[above * 2 + c], above * 2 + c, RING - step, 2)
            swap(step)
        else:
            for kv in range(2):
                arrived(kv, below * 2 + c)
                push(kv, bufs[kv].at[below * 2 + c], below * 2 + c, 4, 2)
        for chunk in (below, above) if step < 4 else (below,):
            for kv in range(2):
                arrived(kv, chunk * 2 + (1 - c))

            @pl.when(chunk <= y)
            def _():
                attend(chunk)

    attended = (acc_ref[...] / l_ref[...]).astype(BF)
    for n in range(4):
        cols = slice(n * 512, (n + 1) * 512)
        term = jnp.dot(attended, wo_ref[:, cols], preferred_element_type=F32)
        out_ref[:, cols] = term.astype(BF)
    for copy in pending:
        copy.wait_send()
    for copy in wcopies:
        copy.wait()


def mix_heads_kernel(
    ht_ref, res_ref, gain_ref, meta_ref, stream_ref, gy_ref,
    xin, part, zin, nbuf, gbuf,
    s1, s3, rx, rz, sy, ry,
):
    a = lax.axis_index("attn")
    e = lax.axis_index("expert")
    y = a // 2
    c = a % 2
    z = e // XS
    x = e % XS
    xs = [(x + d) % XS for d in range(XS)]
    zs = [((z + r) % RING) for r in range(RING)]
    ys = [((y + r) % RING) for r in range(RING)]
    peers = [{"expert": z * XS + xs[d]} for d in range(1, XS)]
    peers += [{"expert": zs[r] * XS + x} for r in range(1, RING)]
    peers += [{"attn": ys[r] * 2 + c} for r in range(1, RING)]
    greet(peers)
    pending = []

    def push(*args, **dev):
        copy = remote(*args, **dev)
        copy.start()
        pending.append(copy)

    def got(buf, sem):
        remote(buf, buf, sem, sem, expert=z * XS + xs[1]).wait_recv()

    for r in ORDER:
        for d in (2, 1, 3):
            push(
                ht_ref.at[zs[r], xs[d]], xin.at[r, d - 1], s1.at[r, d - 1], rx.at[r, d - 1],
                expert=z * XS + xs[d],
            )
    total = res_ref[...].astype(F32)
    for r in ORDER:
        summed = ht_ref[pl.ds(zs[r], 1), pl.ds(x, 1)].reshape(8, D).astype(F32)
        for d in range(XS - 1):
            got(xin.at[r, d], rx.at[r, d])
            summed = summed + xin[r, d].astype(F32)
        if r == 0:
            total = total + summed
        else:
            part[r] = summed.astype(BF)
            push(part.at[r], zin.at[r], s3.at[r], rz.at[r], expert=zs[r] * XS + x)
    for r in ORDER[:-1]:
        got(zin.at[r], rz.at[r])
        total = total + zin[r].astype(F32)
    mean = jnp.mean(total * total, axis=1, keepdims=True)
    normalized = (total * lax.rsqrt(mean + 1e-06) * gain_ref[...]).astype(BF)
    for p in range(2):
        nbuf[p, :, :W] = normalized[:, p * EX : p * EX + W]
        nbuf[p, :, W:] = meta_ref[...]
    for r in ORDER[:-1]:
        push(nbuf.at[ys[r] % 2], gbuf.at[y], sy.at[r], ry.at[r], attn=ys[r] * 2 + c)
    stream_ref[...] = total
    gbuf[pl.ds(y, 1)] = nbuf[pl.ds(y % 2, 1)]
    for r in range(1, RING):
        src = (y + RING - r) % RING
        got(gbuf.at[src], ry.at[r])
    for n in range(4):
        pair = gbuf[2 * n : 2 * n + 2].astype(F32).reshape(16, TW)
        gy_ref[16 * n : 16 * n + 16, :] = pair.astype(BF)
    for copy in pending:
        copy.wait_send()


def experts_kernel(
    gy_ref, stream_ref, wg_ref, wu_ref, wd_ref, pg_ref, pu_ref, pd_ref,
    out_ref,
    wg, wu, wd, toks, chosen, rows, mrows, act, outs, mouts, madd, fine, back, chi, clo,
    zsum, zgot, zlast, ysum, ygot,
    wsem, tsend, trecv, dsend, drecv, msend, mrecv, nsend, nrecv, bsend, brecv,
    zsend, zrecv, zfin, ysend, yrecv,
):
    a = lax.axis_index("attn")
    e = lax.axis_index("expert")
    y = a // 2
    c = a % 2
    odd = y % 2
    quarter = a // 4
    z = e // XS
    x = e % XS
    xs = [(x + d) % XS for d in range(XS)]
    up = ((z + 1) % RING) * XS + x
    down = ((z + RING - 1) % RING) * XS + x
    ys = [((y + r) % RING) for r in range(RING)]
    mate = (y + 1 - 2 * odd) * 2 + c
    own_cols = pl.ds(pl.multiple_of(odd * EX, 128), W)
    mate_cols = pl.ds(pl.multiple_of((1 - odd) * W, 128), EX)
    shared = pl.ds(pl.multiple_of(odd * (W - EX), 128), EX)
    loads = []
    for n, (mine, theirs, dst) in enumerate(
        ((wg_ref.at[0], pg_ref, wg), (wu_ref.at[0], pu_ref, wu), (wd_ref.at[0], pd_ref, wd))
    ):
        for k, src in enumerate((mine, theirs)):
            span = pl.ds(384 * k, 384)
            if n < 2:
                pairs = (
                    (src.at[own_cols], dst.at[pl.ds(0, W), span]),
                    (src.at[mate_cols], dst.at[pl.ds(W, EX), span]),
                )
            else:
                pairs = (
                    (src.at[:, own_cols], dst.at[span, pl.ds(0, W)]),
                    (src.at[:, mate_cols], dst.at[span, pl.ds(W, EX)]),
                )
            for i, (from_ref, to_ref) in enumerate(pairs):
                load = pltpu.make_async_copy(from_ref, to_ref, wsem.at[4 * n + 2 * k + i])
                load.start()
                loads.append(load)
    peers = [{"expert": z * XS + xs[d]} for d in range(1, XS)]
    peers += [{"expert": up}, {"expert": down}]
    peers += [{"attn": ys[r] * 2 + c} for r in range(1, RING)]
    greet(peers)
    pending = []

    def push(*args, **dev):
        copy = remote(*args, **dev)
        copy.start()
        pending.append(copy)

    def got(buf, sem):
        remote(buf, buf, sem, sem, expert=up).wait_recv()

    def half(ref, slot, h):
        return ref.at[slot, pl.ds(32 * h, 32)]

    for h in range(2):
        own = gy_ref.at[pl.ds(32 * h, 32)]
        push(own, half(toks, 1, h), tsend.at[0, h, 0], trecv.at[1, h], expert=up)
        push(own, half(toks, 7, h), tsend.at[0, h, 1], trecv.at[7, h], expert=down)
    toks[0] = gy_ref[...]

    tok = lax.broadcasted_iota(jnp.int32, (64, 64), 0)
    col = lax.broadcasted_iota(jnp.int32, (64, 64), 1)
    earlier = ((tok // 8 == col // 8) & (col < tok)).astype(F32).astype(BF)
    lane = lax.broadcasted_iota(jnp.int32, (64, 128), 1)

    def choose(s):
        meta = toks[s, :, W:TW].astype(F32)
        high = pltpu.roll(meta, 120, 1)
        low = pltpu.roll(meta, 112, 1)
        hit = jnp.zeros((64, 64), F32)
        whi = jnp.zeros((64, 64), F32)
        wlo = jnp.zeros((64, 64), F32)
        for k in range(XS):
            expert = (4 * (z * XS + k) + quarter).astype(F32)
            match = (meta == expert) & (lane < 8)
            here = col // 16 == k
            hit = jnp.where(here, jnp.sum(jnp.where(match, 1.0, 0.0), 1, keepdims=True), hit)
            whi = jnp.where(here, jnp.sum(jnp.where(match, high, 0.0), 1, keepdims=True), whi)
            wlo = jnp.where(here, jnp.sum(jnp.where(match, low, 0.0), 1, keepdims=True), wlo)
        before = jnp.dot(earlier, hit.astype(BF), preferred_element_type=F32)
        place = (2 * (tok // 8)).astype(F32) + before
        pick = jnp.where((col % 16).astype(F32) == place, hit, 0.0)
        chi[s] = (pick * whi).astype(BF)
        clo[s] = (pick * wlo).astype(BF)
        pick = pick.astype(BF)
        for lo, hi in CUTS:
            got_rows = lax.dot_general(
                pick, toks[s, :, lo:hi], (((0,), (0,)), ((), ())), preferred_element_type=F32
            )
            chosen[s, :, :, lo:hi] = got_rows.astype(BF).reshape(XS, 16, hi - lo)

    def ffn(s):
        block = rows[s].reshape(64, W)
        rest = mrows[s].reshape(64, EX)
        for n in range(3):
            cols = slice(n * 256, (n + 1) * 256)
            gate = jnp.dot(block, wg[:W, cols], preferred_element_type=F32) + jnp.dot(
                rest, wg[W:, cols], preferred_element_type=F32
            )
            lift = jnp.dot(block, wu[:W, cols], preferred_element_type=F32) + jnp.dot(
                rest, wu[W:, cols], preferred_element_type=F32
            )
            act[:, cols] = (gate / (1.0 + jnp.exp(-gate)) * lift).astype(BF)
        made = jnp.dot(act[...], wd[:, W:], preferred_element_type=F32)
        mouts[s] = made.astype(BF).reshape(XS, 16, EX)
        push(mouts.at[s], madd.at[s], nsend.at[s], nrecv.at[s], attn=mate)
        for lo, hi in CUTS:
            made = jnp.dot(act[...], wd[:, lo:hi], preferred_element_type=F32)
            fine[s, :, lo:hi] = made

    def spread(s, src, dst, ss, rr):
        for d in (2, 1, 3):
            push(
                src.at[s, xs[d]], dst.at[s, x], ss.at[s, d - 1], rr.at[s, x],
                expert=z * XS + xs[d],
            )

    def gathered(s, buf, rr):
        for d in (1, 3, 2):
            got(buf.at[s, xs[d]], rr.at[s, xs[d]])

    for n in range(RING + 6):
        if n < RING:
            s = SLOTS[n]
            if s:
                for h in range(2):
                    got(half(toks, s, h), trecv.at[s, h])
                    if s < 3 or (s == 3 and h == 0):
                        push(
                            half(toks, s, h), half(toks, s + 1, h), tsend.at[s, h, 0],
                            trecv.at[s + 1, h], expert=up,
                        )
                    if s > 5 or (s == 5 and h == 1):
                        push(
                            half(toks, s, h), half(toks, s - 1, h), tsend.at[s, h, 1],
                            trecv.at[s - 1, h], expert=down,
                        )
            choose(s)
            spread(s, chosen, rows, dsend, drecv)
            rows[s, pl.ds(x, 1)] = chosen[s, pl.ds(x, 1)]
        if 2 <= n < RING + 2:
            s = SLOTS[n - 2]
            gathered(s, rows, drecv)
            push(rows.at[s, :, :, shared], mrows.at[s], msend.at[s], mrecv.at[s], attn=mate)
        if 4 <= n < RING + 4:
            s = SLOTS[n - 4]
            got(mrows.at[s], mrecv.at[s])
            if n == 4:
                for load in loads:
                    load.wait()
            ffn(s)
        if 6 <= n:
            s = SLOTS[n - 6]
            got(madd.at[s], nrecv.at[s])
            fine[s, :, shared] = fine[s, :, shared] + madd[s].reshape(64, EX).astype(F32)
            outs[s] = fine[s].astype(BF).reshape(XS, 16, W)
            spread(s, outs, back, bsend, brecv)
            back[s, pl.ds(x, 1)] = outs[s, pl.ds(x, 1)]

    def combine(s, h):
        part = slice(32 * h, 32 * h + 32)
        made = back[s].reshape(64, W)
        return jnp.dot(chi[s, part, :], made, preferred_element_type=F32) + jnp.dot(
            clo[s, part, :], made, preferred_element_type=F32
        )

    for s in reversed(SLOTS):
        gathered(s, back, brecv)
        for h in range(2):
            value = combine(s, h)
            part = slice(32 * h, 32 * h + 32)
            if s == 0:
                for way in range(2):
                    got(zlast.at[way, pl.ds(32 * h, 32)], zfin.at[way, h])
                    value = value + zlast[way, part, :].astype(F32)
                for j in range(4):
                    row = 4 * h + j
                    ysum[row] = value[8 * j : 8 * j + 8].astype(BF)
                continue
            if s in (1, 2, 6, 7) or (s == 3 and h == 0) or (s == 5 and h == 1):
                got(half(zgot, s, h), zrecv.at[s, h])
                value = value + zgot[s, part, :].astype(F32)
            zsum[s, part, :] = value.astype(BF)
            downward = s < 4 or (s == 4 and h == 0)
            to = s - 1 if downward else (s + 1) % RING
            if to == 0:
                way = 0 if downward else 1
                push(
                    half(zsum, s, h), zlast.at[way, pl.ds(32 * h, 32)], zsend.at[s, h],
                    zfin.at[way, h], expert=down if downward else up,
                )
            else:
                push(
                    half(zsum, s, h), half(zgot, to, h), zsend.at[s, h], zrecv.at[to, h],
                    expert=down if downward else up,
                )
    for r in ORDER[:-1]:
        push(ysum.at[ys[r]], ygot.at[r], ysend.at[r], yrecv.at[r], attn=ys[r] * 2 + c)
    same = ysum[pl.ds(y, 1)].reshape(8, W).astype(F32)
    other = jnp.zeros((8, W), F32)
    for r in range(1, RING):
        got(ygot.at[r], yrecv.at[r])
        if r % 2 == 0:
            same = same + ygot[r].astype(F32)
        else:
            other = other + ygot[r].astype(F32)
    evens = jnp.where(odd == 0, same, other)
    odds = jnp.where(odd == 0, other, same)
    out_ref[:, :EX] = (stream_ref[:, :EX] + evens[:, :EX]).astype(BF)
    out_ref[:, EX:W] = (stream_ref[:, EX:W] + evens[:, EX:] + odds[:, : W - EX]).astype(BF)
    out_ref[:, W:] = (stream_ref[:, W:] + odds[:, W - EX :]).astype(BF)
    for copy in pending:
        copy.wait_send()


def vmem(*shape, dtype=BF):
    return VM(shape, dtype)


def local(
    queries, keys, values, residual, prompt_lengths, out_proj, norm_gain,
    expert_ids, route_weights, w_gate, w_up, w_down,
):
    inv = pl.BlockSpec(memory_space=VM)
    anyw = pl.BlockSpec(memory_space=pl.ANY)
    smem = pl.BlockSpec(memory_space=pltpu.SMEM)
    high = lax.reduce_precision(route_weights, 8, 7)
    low = route_weights - high
    meta = jnp.concatenate(
        [expert_ids.astype(F32), high, low, jnp.zeros((8, 104), F32)], axis=1
    ).astype(BF)

    terms, pg, pu, pd = pl.pallas_call(
        attention_kernel,
        out_shape=(
            jax.ShapeDtypeStruct((256, D), BF),
            jax.ShapeDtypeStruct((D, 384), BF),
            jax.ShapeDtypeStruct((D, 384), BF),
            jax.ShapeDtypeStruct((384, D), BF),
        ),
        in_specs=[smem, inv, inv, inv, inv, anyw, anyw, anyw],
        out_specs=(inv, anyw, anyw, anyw),
        scratch_shapes=[
            vmem(16, 256, 128),
            vmem(16, 256, 128),
            vmem(256, 1, dtype=F32),
            vmem(256, 1, dtype=F32),
            vmem(256, 128, dtype=F32),
            DMA((2, 8, 3)),
            DMA((2, 16)),
            DMA((3, 4)),
            DMA((3, 4)),
        ],
        compiler_params=pltpu.CompilerParams(collective_id=0, has_side_effects=True),
        name="attention",
    )(prompt_lengths, queries, keys, values, out_proj, w_gate, w_up, w_down)

    stream, rows = pl.pallas_call(
        mix_heads_kernel,
        out_shape=(jax.ShapeDtypeStruct((8, D), F32), jax.ShapeDtypeStruct((64, TW), BF)),
        in_specs=[inv] * 4,
        out_specs=(inv, inv),
        scratch_shapes=[vmem(8, 3, 8, D), vmem(8, 8, D), vmem(8, 8, D)]
        + [vmem(2, 8, TW), vmem(8, 8, TW)]
        + [DMA((8, 3)), DMA((8,)), DMA((8, 3)), DMA((8,)), DMA((8,)), DMA((8,))],
        compiler_params=pltpu.CompilerParams(collective_id=1, has_side_effects=True),
        name="mix_heads",
    )(terms.reshape(8, 4, 8, D), residual, norm_gain.reshape(1, D), meta)

    return pl.pallas_call(
        experts_kernel,
        out_shape=jax.ShapeDtypeStruct((8, D), BF),
        in_specs=[inv, inv] + [anyw] * 6,
        out_specs=inv,
        scratch_shapes=[
            vmem(D, 768),
            vmem(D, 768),
            vmem(768, D),
            vmem(8, 64, TW),
            vmem(8, 4, 16, W),
            vmem(8, 4, 16, W),
            vmem(8, 4, 16, EX),
            vmem(64, 768),
            vmem(8, 4, 16, W),
            vmem(8, 4, 16, EX),
            vmem(8, 4, 16, EX),
            vmem(8, 64, W, dtype=F32),
            vmem(8, 4, 16, W),
            vmem(8, 64, 64),
            vmem(8, 64, 64),
            vmem(8, 64, W),
            vmem(8, 64, W),
            vmem(2, 64, W),
            vmem(8, 8, W),
            vmem(8, 8, W),
            DMA((12,)),
            DMA((8, 2, 2)),
            DMA((8, 2)),
            DMA((8, 3)),
            DMA((8, 4)),
            DMA((8,)),
            DMA((8,)),
            DMA((8,)),
            DMA((8,)),
            DMA((8, 3)),
            DMA((8, 4)),
            DMA((8, 2)),
            DMA((8, 2)),
            DMA((2, 2)),
            DMA((8,)),
            DMA((8,)),
        ],
        compiler_params=pltpu.CompilerParams(collective_id=2, has_side_effects=True),
        name="experts",
    )(rows, stream, w_gate, w_up, w_down, pg, pu, pd)


def solution(mesh):
    return jax.shard_map(
        local,
        mesh=mesh,
        in_specs=(
            P("attn", "expert"),
            P(None, "attn", None),
            P(None, "attn", None),
            P(("attn", "expert"), None),
            P(),
            P("expert", None),
            P(),
            P(("attn", "expert"), None),
            P(("attn", "expert"), None),
            P("expert", None, "attn"),
            P("expert", None, "attn"),
            P("expert", "attn", None),
        ),
        out_specs=P(("attn", "expert"), None),
        check_vma=False,
    )
```

```python
import math

import jax
import jax.numpy as jnp
from jax import lax
from jax.experimental import pallas as pl
from jax.experimental.pallas import tpu as pltpu
from jax.sharding import PartitionSpec as P

BF = jnp.bfloat16
F32 = jnp.float32
VM = pltpu.VMEM
DMA = pltpu.SemaphoreType.DMA
D = 2048
EX = 640
W = D - EX
TW = W + 128
CUTS = ((0, 512), (512, 1024), (1024, W))
RING = 8
XS = 4
QSCALE = math.log2(math.e) / math.sqrt(128.0)
ORDER = (4, 3, 5, 2, 6, 1, 7, 0)
SLOTS = (0, 1, 7, 2, 6, 3, 5, 4)


def remote(src, dst, send, recv, **dev):
    return pltpu.make_async_remote_copy(
        src_ref=src,
        dst_ref=dst,
        send_sem=send,
        recv_sem=recv,
        device_id=dev,
        device_id_type=pl.DeviceIdType.MESH,
    )


def greet(peers):
    barrier = pltpu.get_barrier_semaphore()
    for peer in peers:
        pl.semaphore_signal(barrier, inc=1, device_id=peer, device_id_type=pl.DeviceIdType.MESH)
    pl.semaphore_wait(barrier, len(peers))


def attention_stage(
    lengths, q_ref, k_ref, v_ref, att_ref, kbuf, vbuf, m_ref, l_ref, acc_ref, send, recv, pending
):
    a = lax.axis_index("attn")
    e = lax.axis_index("expert")
    y = a // 2
    c = a % 2
    head = e // 16
    right = ((y + 1) % RING) * 2 + c
    left = ((y + RING - 1) % RING) * 2 + c
    partner = y * 2 + (1 - c)
    bufs = (kbuf, vbuf)
    ins = (k_ref, v_ref)

    def push(kv, src, block, slot, way):
        to = (right, left, partner)[way]
        copy = remote(
            src, bufs[kv].at[block], send.at[kv, slot, way], recv.at[kv, block], attn=to
        )
        copy.start()
        pending.append(copy)

    def arrived(kv, block):
        remote(
            bufs[kv].at[block], bufs[kv].at[block], send.at[kv, 0, 0], recv.at[kv, block],
            attn=partner,
        ).wait_recv()

    for way in (2, 0, 1):
        for kv in range(2):
            push(kv, ins[kv].at[head], a, 0, way)
    kbuf[pl.ds(a, 1)] = k_ref[pl.ds(head, 1)]
    vbuf[pl.ds(a, 1)] = v_ref[pl.ds(head, 1)]

    end1 = lengths[0]
    end2 = end1 + lengths[1]
    end3 = end2 + lengths[2]
    qpos = a * 256 + lax.broadcasted_iota(jnp.int32, (256, 1), 0)
    first = jnp.where(
        qpos >= end3, end3, jnp.where(qpos >= end2, end2, jnp.where(qpos >= end1, end1, 0))
    )
    m_ref[...] = jnp.full((256, 1), -1e30, F32)
    l_ref[...] = jnp.zeros((256, 1), F32)
    acc_ref[...] = jnp.zeros((256, 128), F32)

    def attend(chunk):
        kc = kbuf[pl.ds(chunk * 2, 2)].reshape(512, 128)
        vc = vbuf[pl.ds(chunk * 2, 2)].reshape(512, 128)
        scores = lax.dot_general(
            q_ref[...], kc, (((1,), (1,)), ((), ())), preferred_element_type=F32
        )
        kpos = chunk * 512 + lax.broadcasted_iota(jnp.int32, (256, 512), 1)
        scores = jnp.where((kpos >= first) & (kpos <= qpos), scores * QSCALE, -1e30)
        old = m_ref[...]
        new = jnp.maximum(old, jnp.max(scores, axis=1, keepdims=True))
        factor = jnp.exp2(old - new)
        weights = jnp.exp2(scores - new)
        m_ref[...] = new
        l_ref[...] = l_ref[...] * factor + jnp.sum(weights, axis=1, keepdims=True)
        acc_ref[...] = acc_ref[...] * factor + jnp.dot(
            weights.astype(BF), vc, preferred_element_type=F32
        )

    for kv in range(2):
        arrived(kv, partner)
    attend(y)
    for step in range(1, 5):
        below = (y + RING - step) % RING
        above = (y + step) % RING
        if step < 4:
            for kv in range(2):
                arrived(kv, below * 2 + c)
                if step < 3 or kv == 0:
                    push(kv, bufs[kv].at[below * 2 + c], below * 2 + c, step, 0)
                push(kv, bufs[kv].at[below * 2 + c], below * 2 + c, step, 2)
            for kv in range(2):
                arrived(kv, above * 2 + c)
                if step < 3 or kv == 1:
                    push(kv, bufs[kv].at[above * 2 + c], above * 2 + c, RING - step, 1)
                push(kv, bufs[kv].at[above * 2 + c], above * 2 + c, RING - step, 2)
        else:
            for kv in range(2):
                arrived(kv, below * 2 + c)
                push(kv, bufs[kv].at[below * 2 + c], below * 2 + c, 4, 2)
        for chunk in (below, above) if step < 4 else (below,):
            for kv in range(2):
                arrived(kv, chunk * 2 + (1 - c))

            @pl.when(chunk <= y)
            def _():
                attend(chunk)

    att_ref[...] = (acc_ref[...] / l_ref[...]).astype(BF)


def mix_stage(
    att_ref, wo_ref, res_ref, gain_ref, ids_ref, gates_ref, stream_ref, toks,
    ht_ref, xin, part, zin, nbuf, gbuf, s1, s3, rx, rz, sy, ry, pending,
):
    a = lax.axis_index("attn")
    e = lax.axis_index("expert")
    y = a // 2
    c = a % 2
    z = e // XS
    x = e % XS
    xs = [(x + d) % XS for d in range(XS)]
    zs = [((z + r) % RING) for r in range(RING)]
    ys = [((y + r) % RING) for r in range(RING)]

    def push(*args, **dev):
        copy = remote(*args, **dev)
        copy.start()
        pending.append(copy)

    def got(buf, sem):
        remote(buf, buf, sem, sem, expert=z * XS + xs[1]).wait_recv()

    for r in ORDER:
        part_rows = att_ref[pl.ds(pl.multiple_of(zs[r] * 32, 32), 32)]
        for n in range(4):
            cols = slice(n * 512, (n + 1) * 512)
            term = jnp.dot(part_rows, wo_ref[:, cols], preferred_element_type=F32)
            ht_ref[pl.ds(zs[r], 1), :, :, cols] = term.reshape(1, XS, 8, 512).astype(BF)
        for d in (2, 1, 3):
            push(
                ht_ref.at[zs[r], xs[d]], xin.at[r, d - 1], s1.at[r, d - 1], rx.at[r, d - 1],
                expert=z * XS + xs[d],
            )
    total = res_ref[...].astype(F32)
    for r in ORDER:
        summed = ht_ref[pl.ds(zs[r], 1), pl.ds(x, 1)].reshape(8, D).astype(F32)
        for d in range(XS - 1):
            got(xin.at[r, d], rx.at[r, d])
            summed = summed + xin[r, d].astype(F32)
        if r == 0:
            total = total + summed
        else:
            part[r] = summed.astype(BF)
            push(part.at[r], zin.at[r], s3.at[r], rz.at[r], expert=zs[r] * XS + x)
    for r in ORDER[:-1]:
        got(zin.at[r], rz.at[r])
        total = total + zin[r].astype(F32)
    mean = jnp.mean(total * total, axis=1, keepdims=True)
    normalized = (total * lax.rsqrt(mean + 1e-06) * gain_ref[...]).astype(BF)
    weight = gates_ref[...]
    high = weight.astype(BF)
    low = (weight - high.astype(F32)).astype(BF)
    for p in range(2):
        nbuf[p, :, W:] = jnp.zeros((8, 128), BF)
        nbuf[p, :, W : W + 8] = ids_ref[...].astype(F32).astype(BF)
        nbuf[p, :, W + 8 : W + 16] = high
        nbuf[p, :, W + 16 : W + 24] = low
        nbuf[p, :, :W] = normalized[:, p * EX : p * EX + W]
    for r in ORDER[:-1]:
        push(nbuf.at[ys[r] % 2], gbuf.at[y], sy.at[r], ry.at[r], attn=ys[r] * 2 + c)
    stream_ref[...] = total
    gbuf[pl.ds(y, 1)] = nbuf[pl.ds(y % 2, 1)]
    for r in range(1, RING):
        src = (y + RING - r) % RING
        got(gbuf.at[src], ry.at[r])
    for n in range(4):
        pair = gbuf[2 * n : 2 * n + 2].astype(F32).reshape(16, TW)
        toks[0, 16 * n : 16 * n + 16, :] = pair.astype(BF)


def experts_stage(
    stream_ref, out_ref, wg, wu, wd, loads,
    toks, chosen, rows, mrows, act, outs, mouts, madd, fine, back, chi, clo,
    zsum, zgot, zlast, ysum, ygot,
    tsend, trecv, dsend, drecv, msend, mrecv, nsend, nrecv, bsend, brecv,
    zsend, zrecv, zfin, ysend, yrecv, pending,
):
    a = lax.axis_index("attn")
    e = lax.axis_index("expert")
    y = a // 2
    c = a % 2
    odd = y % 2
    quarter = a // 4
    z = e // XS
    x = e % XS
    xs = [(x + d) % XS for d in range(XS)]
    up = ((z + 1) % RING) * XS + x
    down = ((z + RING - 1) % RING) * XS + x
    ys = [((y + r) % RING) for r in range(RING)]
    mate = (y + 1 - 2 * odd) * 2 + c
    shared = pl.ds(pl.multiple_of(odd * (W - EX), 128), EX)

    def push(*args, **dev):
        copy = remote(*args, **dev)
        copy.start()
        pending.append(copy)

    def got(buf, sem):
        remote(buf, buf, sem, sem, expert=up).wait_recv()

    def half(ref, slot, h):
        return ref.at[slot, pl.ds(32 * h, 32)]

    for h in range(2):
        own = half(toks, 0, h)
        push(own, half(toks, 1, h), tsend.at[0, h, 0], trecv.at[1, h], expert=up)
        push(own, half(toks, 7, h), tsend.at[0, h, 1], trecv.at[7, h], expert=down)

    tok = lax.broadcasted_iota(jnp.int32, (64, 64), 0)
    col = lax.broadcasted_iota(jnp.int32, (64, 64), 1)
    earlier = ((tok // 8 == col // 8) & (col < tok)).astype(F32).astype(BF)
    lane = lax.broadcasted_iota(jnp.int32, (64, 128), 1)

    def choose(s):
        meta = toks[s, :, W:TW].astype(F32)
        high = pltpu.roll(meta, 120, 1)
        low = pltpu.roll(meta, 112, 1)
        hit = jnp.zeros((64, 64), F32)
        whi = jnp.zeros((64, 64), F32)
        wlo = jnp.zeros((64, 64), F32)
        for k in range(XS):
            expert = (4 * (z * XS + k) + quarter).astype(F32)
            match = (meta == expert) & (lane < 8)
            here = col // 16 == k
            hit = jnp.where(here, jnp.sum(jnp.where(match, 1.0, 0.0), 1, keepdims=True), hit)
            whi = jnp.where(here, jnp.sum(jnp.where(match, high, 0.0), 1, keepdims=True), whi)
            wlo = jnp.where(here, jnp.sum(jnp.where(match, low, 0.0), 1, keepdims=True), wlo)
        before = jnp.dot(earlier, hit.astype(BF), preferred_element_type=F32)
        place = (2 * (tok // 8)).astype(F32) + before
        pick = jnp.where((col % 16).astype(F32) == place, hit, 0.0)
        chi[s] = (pick * whi).astype(BF)
        clo[s] = (pick * wlo).astype(BF)
        pick = pick.astype(BF)
        for lo, hi in CUTS:
            got_rows = lax.dot_general(
                pick, toks[s, :, lo:hi], (((0,), (0,)), ((), ())), preferred_element_type=F32
            )
            chosen[s, :, :, lo:hi] = got_rows.astype(BF).reshape(XS, 16, hi - lo)

    def ffn(s):
        block = rows[s].reshape(64, W)
        rest = mrows[s].reshape(64, EX)
        for n in range(3):
            cols = slice(n * 256, (n + 1) * 256)
            gate = jnp.dot(block, wg[:W, cols], preferred_element_type=F32) + jnp.dot(
                rest, wg[W:, cols], preferred_element_type=F32
            )
            lift = jnp.dot(block, wu[:W, cols], preferred_element_type=F32) + jnp.dot(
                rest, wu[W:, cols], preferred_element_type=F32
            )
            act[:, cols] = (gate / (1.0 + jnp.exp(-gate)) * lift).astype(BF)
        made = jnp.dot(act[...], wd[:, W:], preferred_element_type=F32)
        mouts[s] = made.astype(BF).reshape(XS, 16, EX)
        push(mouts.at[s], madd.at[s], nsend.at[s], nrecv.at[s], attn=mate)
        for lo, hi in CUTS:
            made = jnp.dot(act[...], wd[:, lo:hi], preferred_element_type=F32)
            fine[s, :, lo:hi] = made

    def spread(s, src, dst, ss, rr):
        for d in (2, 1, 3):
            push(
                src.at[s, xs[d]], dst.at[s, x], ss.at[s, d - 1], rr.at[s, x],
                expert=z * XS + xs[d],
            )

    def gathered(s, buf, rr):
        for d in (1, 3, 2):
            got(buf.at[s, xs[d]], rr.at[s, xs[d]])

    for n in range(RING + 6):
        if n < RING:
            s = SLOTS[n]
            if s:
                for h in range(2):
                    got(half(toks, s, h), trecv.at[s, h])
                    if s < 3 or (s == 3 and h == 0):
                        push(
                            half(toks, s, h), half(toks, s + 1, h), tsend.at[s, h, 0],
                            trecv.at[s + 1, h], expert=up,
                        )
                    if s > 5 or (s == 5 and h == 1):
                        push(
                            half(toks, s, h), half(toks, s - 1, h), tsend.at[s, h, 1],
                            trecv.at[s - 1, h], expert=down,
                        )
            choose(s)
            spread(s, chosen, rows, dsend, drecv)
            rows[s, pl.ds(x, 1)] = chosen[s, pl.ds(x, 1)]
        if 2 <= n < RING + 2:
            s = SLOTS[n - 2]
            gathered(s, rows, drecv)
            push(rows.at[s, :, :, shared], mrows.at[s], msend.at[s], mrecv.at[s], attn=mate)
        if 4 <= n < RING + 4:
            s = SLOTS[n - 4]
            got(mrows.at[s], mrecv.at[s])
            if n == 4:
                for load in loads:
                    load.wait()
            ffn(s)
        if 6 <= n:
            s = SLOTS[n - 6]
            got(madd.at[s], nrecv.at[s])
            fine[s, :, shared] = fine[s, :, shared] + madd[s].reshape(64, EX).astype(F32)
            outs[s] = fine[s].astype(BF).reshape(XS, 16, W)
            spread(s, outs, back, bsend, brecv)
            back[s, pl.ds(x, 1)] = outs[s, pl.ds(x, 1)]

    def combine(s, h):
        part = slice(32 * h, 32 * h + 32)
        made = back[s].reshape(64, W)
        return jnp.dot(chi[s, part, :], made, preferred_element_type=F32) + jnp.dot(
            clo[s, part, :], made, preferred_element_type=F32
        )

    for s in reversed(SLOTS):
        gathered(s, back, brecv)
        for h in range(2):
            value = combine(s, h)
            part = slice(32 * h, 32 * h + 32)
            if s == 0:
                for way in range(2):
                    got(zlast.at[way, pl.ds(32 * h, 32)], zfin.at[way, h])
                    value = value + zlast[way, part, :].astype(F32)
                for j in range(4):
                    row = 4 * h + j
                    ysum[row] = value[8 * j : 8 * j + 8].astype(BF)
                continue
            if s in (1, 2, 6, 7) or (s == 3 and h == 0) or (s == 5 and h == 1):
                got(half(zgot, s, h), zrecv.at[s, h])
                value = value + zgot[s, part, :].astype(F32)
            zsum[s, part, :] = value.astype(BF)
            downward = s < 4 or (s == 4 and h == 0)
            to = s - 1 if downward else (s + 1) % RING
            if to == 0:
                way = 0 if downward else 1
                push(
                    half(zsum, s, h), zlast.at[way, pl.ds(32 * h, 32)], zsend.at[s, h],
                    zfin.at[way, h], expert=down if downward else up,
                )
            else:
                push(
                    half(zsum, s, h), half(zgot, to, h), zsend.at[s, h], zrecv.at[to, h],
                    expert=down if downward else up,
                )
    for r in ORDER[:-1]:
        push(ysum.at[ys[r]], ygot.at[r], ysend.at[r], yrecv.at[r], attn=ys[r] * 2 + c)
    same = ysum[pl.ds(y, 1)].reshape(8, W).astype(F32)
    other = jnp.zeros((8, W), F32)
    for r in range(1, RING):
        got(ygot.at[r], yrecv.at[r])
        if r % 2 == 0:
            same = same + ygot[r].astype(F32)
        else:
            other = other + ygot[r].astype(F32)
    evens = jnp.where(odd == 0, same, other)
    odds = jnp.where(odd == 0, other, same)
    out_ref[:, :EX] = (stream_ref[:, :EX] + evens[:, :EX]).astype(BF)
    out_ref[:, EX:W] = (stream_ref[:, EX:W] + evens[:, EX:] + odds[:, : W - EX]).astype(BF)
    out_ref[:, W:] = (stream_ref[:, W:] + odds[:, W - EX :]).astype(BF)


def layer_kernel(
    lengths, q_ref, k_ref, v_ref, wo_ref, wg_ref, wu_ref, wd_ref, res_ref, gain_ref,
    ids_ref, gates_ref, out_ref,
    kbuf, vbuf, m_ref, l_ref, acc_ref, att_ref, send, recv,
    stream_ref, ht_ref, xin, part, zin, nbuf, gbuf, s1, s3, rx, rz, sy, ry,
    wg, wu, wd, wsem, wsend, wrecv, toks, *rest,
):
    a = lax.axis_index("attn")
    e = lax.axis_index("expert")
    y = a // 2
    c = a % 2
    odd = y % 2
    z = e // XS
    x = e % XS
    partner = y * 2 + (1 - c)
    own_cols = pl.ds(pl.multiple_of(odd * EX, 128), W)
    mate_cols = pl.ds(pl.multiple_of((1 - odd) * W, 128), EX)
    moves = []
    for n, (src, dst) in enumerate(((wg_ref.at[0], wg), (wu_ref.at[0], wu), (wd_ref.at[0], wd))):
        for i, (take, put) in enumerate(((own_cols, pl.ds(0, W)), (mate_cols, pl.ds(W, EX)))):
            for k in range(2):
                span = pl.ds(384 * k, 384)
                moves.append(
                    (2 * n + i, k, src.at[take], dst.at[put, span])
                    if n < 2
                    else (2 * n + i, k, src.at[:, take], dst.at[span, put])
                )
    loads = []
    for n, k, src, dst in moves:
        if k == 0:
            load = pltpu.make_async_copy(src, dst, wsem.at[n])
            load.start()
            loads.append(load)
    peers = [{"attn": partner}]
    peers += [{"attn": (y + r) % RING * 2 + c} for r in range(1, RING)]
    peers += [{"expert": (z + r) % RING * XS + x} for r in range(1, RING)]
    peers += [{"expert": z * XS + (x + d) % XS} for d in range(1, XS)]
    greet(peers)
    pending = []
    attention_stage(
        lengths, q_ref, k_ref, v_ref, att_ref, kbuf, vbuf, m_ref, l_ref, acc_ref, send, recv,
        pending,
    )
    for n, k, src, dst in moves:
        if k == 1:
            swap = remote(src, dst, wsend.at[n], wrecv.at[n], attn=partner)
            swap.start()
            loads.append(swap)
    mix_stage(
        att_ref, wo_ref, res_ref, gain_ref, ids_ref, gates_ref, stream_ref, toks,
        ht_ref, xin, part, zin, nbuf, gbuf, s1, s3, rx, rz, sy, ry, pending,
    )
    experts_stage(stream_ref, out_ref, wg, wu, wd, loads, toks, *rest, pending)
    for copy in pending:
        copy.wait_send()


def vmem(*shape, dtype=BF):
    return VM(shape, dtype)


def local(
    queries, keys, values, residual, prompt_lengths, out_proj, norm_gain,
    expert_ids, route_weights, w_gate, w_up, w_down,
):
    inv = pl.BlockSpec(memory_space=VM)
    anyw = pl.BlockSpec(memory_space=pl.ANY)
    smem = pl.BlockSpec(memory_space=pltpu.SMEM)
    return pl.pallas_call(
        layer_kernel,
        out_shape=jax.ShapeDtypeStruct((8, D), BF),
        in_specs=[smem, inv, inv, inv, inv, anyw, anyw, anyw, inv, inv, inv, inv],
        out_specs=inv,
        scratch_shapes=[
            vmem(16, 256, 128),
            vmem(16, 256, 128),
            vmem(256, 1, dtype=F32),
            vmem(256, 1, dtype=F32),
            vmem(256, 128, dtype=F32),
            vmem(256, 128),
            DMA((2, 8, 3)),
            DMA((2, 16)),
            vmem(8, D, dtype=F32),
            vmem(8, 4, 8, D),
            vmem(8, 3, 8, D),
            vmem(8, 8, D),
            vmem(8, 8, D),
            vmem(2, 8, TW),
            vmem(8, 8, TW),
            DMA((8, 3)),
            DMA((8,)),
            DMA((8, 3)),
            DMA((8,)),
            DMA((8,)),
            DMA((8,)),
            vmem(D, 768),
            vmem(D, 768),
            vmem(768, D),
            DMA((6,)),
            DMA((6,)),
            DMA((6,)),
            vmem(8, 64, TW),
            vmem(8, 4, 16, W),
            vmem(8, 4, 16, W),
            vmem(8, 4, 16, EX),
            vmem(64, 768),
            vmem(8, 4, 16, W),
            vmem(8, 4, 16, EX),
            vmem(8, 4, 16, EX),
            vmem(8, 64, W, dtype=F32),
            vmem(8, 4, 16, W),
            vmem(8, 64, 64),
            vmem(8, 64, 64),
            vmem(8, 64, W),
            vmem(8, 64, W),
            vmem(2, 64, W),
            vmem(8, 8, W),
            vmem(8, 8, W),
            DMA((8, 2, 2)),
            DMA((8, 2)),
            DMA((8, 3)),
            DMA((8, 4)),
            DMA((8,)),
            DMA((8,)),
            DMA((8,)),
            DMA((8,)),
            DMA((8, 3)),
            DMA((8, 4)),
            DMA((8, 2)),
            DMA((8, 2)),
            DMA((2, 2)),
            DMA((8,)),
            DMA((8,)),
        ],
        compiler_params=pltpu.CompilerParams(collective_id=0, has_side_effects=True),
        name="layer",
    )(
        prompt_lengths, queries, keys, values, out_proj, w_gate, w_up, w_down,
        residual, norm_gain.reshape(1, D), expert_ids, route_weights,
    )


def solution(mesh):
    return jax.shard_map(
        local,
        mesh=mesh,
        in_specs=(
            P("attn", "expert"),
            P(None, "attn", None),
            P(None, "attn", None),
            P(("attn", "expert"), None),
            P(),
            P("expert", None),
            P(),
            P(("attn", "expert"), None),
            P(("attn", "expert"), None),
            P("expert", None, "attn"),
            P("expert", None, "attn"),
            P("expert", "attn", None),
        ),
        out_specs=P(("attn", "expert"), None),
        check_vma=False,
    )
```

```python
import math

import jax
import jax.numpy as jnp
from jax import lax
from jax.experimental import pallas as pl
from jax.experimental.pallas import tpu as pltpu
from jax.sharding import PartitionSpec as P

BF = jnp.bfloat16
F32 = jnp.float32
VM = pltpu.VMEM
DMA = pltpu.SemaphoreType.DMA
D = 2048
EX = 768
W = D - EX
TW = W + 128
CUTS = ((0, 512), (512, 1024), (1024, W))
RING = 8
XS = 4
QSCALE = math.log2(math.e) / math.sqrt(128.0)
ORDER = (4, 3, 5, 2, 6, 1, 7, 0)
SLOTS = (0, 1, 7, 2, 6, 3, 5, 4)


def remote(src, dst, send, recv, **dev):
    return pltpu.make_async_remote_copy(
        src_ref=src,
        dst_ref=dst,
        send_sem=send,
        recv_sem=recv,
        device_id=dev,
        device_id_type=pl.DeviceIdType.MESH,
    )


def greet(peers):
    barrier = pltpu.get_barrier_semaphore()
    for peer in peers:
        pl.semaphore_signal(barrier, inc=1, device_id=peer, device_id_type=pl.DeviceIdType.MESH)
    pl.semaphore_wait(barrier, len(peers))


def attention_stage(
    lengths, q_ref, k_ref, v_ref, att_ref, kbuf, vbuf, m_ref, l_ref, acc_ref, send, recv, pending
):
    a = lax.axis_index("attn")
    e = lax.axis_index("expert")
    y = a // 2
    c = a % 2
    head = e // 16
    right = ((y + 1) % RING) * 2 + c
    left = ((y + RING - 1) % RING) * 2 + c
    partner = y * 2 + (1 - c)
    bufs = (kbuf, vbuf)
    ins = (k_ref, v_ref)

    def push(kv, src, block, slot, way):
        to = (right, left, partner)[way]
        copy = remote(
            src, bufs[kv].at[block], send.at[kv, slot, way], recv.at[kv, block], attn=to
        )
        copy.start()
        pending.append(copy)

    def arrived(kv, block):
        remote(
            bufs[kv].at[block], bufs[kv].at[block], send.at[kv, 0, 0], recv.at[kv, block],
            attn=partner,
        ).wait_recv()

    for way in (2, 0, 1):
        for kv in range(2):
            push(kv, ins[kv].at[head], a, 0, way)
    kbuf[pl.ds(a, 1)] = k_ref[pl.ds(head, 1)]
    vbuf[pl.ds(a, 1)] = v_ref[pl.ds(head, 1)]

    end1 = lengths[0]
    end2 = end1 + lengths[1]
    end3 = end2 + lengths[2]
    qpos = a * 256 + lax.broadcasted_iota(jnp.int32, (256, 1), 0)
    first = jnp.where(
        qpos >= end3, end3, jnp.where(qpos >= end2, end2, jnp.where(qpos >= end1, end1, 0))
    )
    m_ref[...] = jnp.full((256, 1), -1e30, F32)
    l_ref[...] = jnp.zeros((256, 1), F32)
    acc_ref[...] = jnp.zeros((256, 128), F32)

    def attend(chunk):
        kc = kbuf[pl.ds(chunk * 2, 2)].reshape(512, 128)
        vc = vbuf[pl.ds(chunk * 2, 2)].reshape(512, 128)
        scores = lax.dot_general(
            q_ref[...], kc, (((1,), (1,)), ((), ())), preferred_element_type=F32
        )
        kpos = chunk * 512 + lax.broadcasted_iota(jnp.int32, (256, 512), 1)
        scores = jnp.where((kpos >= first) & (kpos <= qpos), scores * QSCALE, -1e30)
        old = m_ref[...]
        new = jnp.maximum(old, jnp.max(scores, axis=1, keepdims=True))
        factor = jnp.exp2(old - new)
        weights = jnp.exp2(scores - new)
        m_ref[...] = new
        l_ref[...] = l_ref[...] * factor + jnp.sum(weights, axis=1, keepdims=True)
        acc_ref[...] = acc_ref[...] * factor + jnp.dot(
            weights.astype(BF), vc, preferred_element_type=F32
        )

    for kv in range(2):
        arrived(kv, partner)
    attend(y)
    for step in range(1, 5):
        below = (y + RING - step) % RING
        above = (y + step) % RING
        if step < 4:
            for kv in range(2):
                arrived(kv, below * 2 + c)
                if step < 3 or kv == 0:
                    push(kv, bufs[kv].at[below * 2 + c], below * 2 + c, step, 0)
                push(kv, bufs[kv].at[below * 2 + c], below * 2 + c, step, 2)
            for kv in range(2):
                arrived(kv, above * 2 + c)
                if step < 3 or kv == 1:
                    push(kv, bufs[kv].at[above * 2 + c], above * 2 + c, RING - step, 1)
                push(kv, bufs[kv].at[above * 2 + c], above * 2 + c, RING - step, 2)
        else:
            for kv in range(2):
                arrived(kv, below * 2 + c)
                push(kv, bufs[kv].at[below * 2 + c], below * 2 + c, 4, 2)
        for chunk in (below, above) if step < 4 else (below,):
            for kv in range(2):
                arrived(kv, chunk * 2 + (1 - c))

            @pl.when(chunk <= y)
            def _():
                attend(chunk)

    att_ref[...] = (acc_ref[...] / l_ref[...]).astype(BF)


def mix_stage(
    att_ref, wo_ref, res_ref, gain_ref, ids_ref, gates_ref, stream_ref, toks,
    ht_ref, xin, part, zin, nbuf, gbuf, s1, s3, rx, rz, sy, ry, pending,
):
    a = lax.axis_index("attn")
    e = lax.axis_index("expert")
    y = a // 2
    c = a % 2
    z = e // XS
    x = e % XS
    xs = [(x + d) % XS for d in range(XS)]
    zs = [((z + r) % RING) for r in range(RING)]
    ys = [((y + r) % RING) for r in range(RING)]

    def push(*args, **dev):
        copy = remote(*args, **dev)
        copy.start()
        pending.append(copy)

    def got(buf, sem):
        remote(buf, buf, sem, sem, expert=z * XS + xs[1]).wait_recv()

    for r in ORDER:
        part_rows = att_ref[pl.ds(pl.multiple_of(zs[r] * 32, 32), 32)]
        for n in range(4):
            cols = slice(n * 512, (n + 1) * 512)
            term = jnp.dot(part_rows, wo_ref[:, cols], preferred_element_type=F32)
            ht_ref[pl.ds(zs[r], 1), :, :, cols] = term.reshape(1, XS, 8, 512).astype(BF)
        for d in (2, 1, 3):
            push(
                ht_ref.at[zs[r], xs[d]], xin.at[r, d - 1], s1.at[r, d - 1], rx.at[r, d - 1],
                expert=z * XS + xs[d],
            )
    total = res_ref[...].astype(F32)
    for r in ORDER:
        summed = ht_ref[pl.ds(zs[r], 1), pl.ds(x, 1)].reshape(8, D).astype(F32)
        for d in range(XS - 1):
            got(xin.at[r, d], rx.at[r, d])
            summed = summed + xin[r, d].astype(F32)
        if r == 0:
            total = total + summed
        else:
            part[r] = summed.astype(BF)
            push(part.at[r], zin.at[r], s3.at[r], rz.at[r], expert=zs[r] * XS + x)
    for r in ORDER[:-1]:
        got(zin.at[r], rz.at[r])
        total = total + zin[r].astype(F32)
    mean = jnp.mean(total * total, axis=1, keepdims=True)
    normalized = (total * lax.rsqrt(mean + 1e-06) * gain_ref[...]).astype(BF)
    weight = gates_ref[...]
    high = weight.astype(BF)
    low = (weight - high.astype(F32)).astype(BF)
    for p in range(2):
        nbuf[p, :, W:] = jnp.zeros((8, 128), BF)
        nbuf[p, :, W : W + 8] = ids_ref[...].astype(F32).astype(BF)
        nbuf[p, :, W + 8 : W + 16] = high
        nbuf[p, :, W + 16 : W + 24] = low
        nbuf[p, :, :W] = normalized[:, p * EX : p * EX + W]
    for r in ORDER[:-1]:
        push(nbuf.at[ys[r] % 2], gbuf.at[y], sy.at[r], ry.at[r], attn=ys[r] * 2 + c)
    stream_ref[...] = total
    gbuf[pl.ds(y, 1)] = nbuf[pl.ds(y % 2, 1)]
    for r in range(1, RING):
        src = (y + RING - r) % RING
        got(gbuf.at[src], ry.at[r])
    for n in range(4):
        pair = gbuf[2 * n : 2 * n + 2].astype(F32).reshape(16, TW)
        toks[0, 16 * n : 16 * n + 16, :] = pair.astype(BF)


def experts_stage(
    stream_ref, out_ref, wg, wu, wd, loads,
    toks, chosen, rows, mrows, act, outs, mouts, madd, fine, back, chi, clo,
    zsum, zgot, zlast, ysum, ygot,
    tsend, trecv, dsend, drecv, msend, mrecv, nsend, nrecv, bsend, brecv,
    zsend, zrecv, zfin, ysend, yrecv, pending,
):
    a = lax.axis_index("attn")
    e = lax.axis_index("expert")
    y = a // 2
    c = a % 2
    odd = y % 2
    quarter = a // 4
    z = e // XS
    x = e % XS
    xs = [(x + d) % XS for d in range(XS)]
    up = ((z + 1) % RING) * XS + x
    down = ((z + RING - 1) % RING) * XS + x
    ys = [((y + r) % RING) for r in range(RING)]
    mate = (y + 1 - 2 * odd) * 2 + c
    shared = pl.ds(pl.multiple_of(odd * (W - EX), 128), EX)

    def push(*args, **dev):
        copy = remote(*args, **dev)
        copy.start()
        pending.append(copy)

    def got(buf, sem):
        remote(buf, buf, sem, sem, expert=up).wait_recv()

    def half(ref, slot, h):
        return ref.at[slot, pl.ds(32 * h, 32)]

    for h in range(2):
        own = half(toks, 0, h)
        push(own, half(toks, 1, h), tsend.at[0, h, 0], trecv.at[1, h], expert=up)
        push(own, half(toks, 7, h), tsend.at[0, h, 1], trecv.at[7, h], expert=down)

    tok = lax.broadcasted_iota(jnp.int32, (64, 64), 0)
    col = lax.broadcasted_iota(jnp.int32, (64, 64), 1)
    earlier = ((tok // 8 == col // 8) & (col < tok)).astype(F32).astype(BF)
    lane = lax.broadcasted_iota(jnp.int32, (64, 128), 1)

    def choose(s):
        meta = toks[s, :, W:TW].astype(F32)
        high = pltpu.roll(meta, 120, 1)
        low = pltpu.roll(meta, 112, 1)
        hit = jnp.zeros((64, 64), F32)
        whi = jnp.zeros((64, 64), F32)
        wlo = jnp.zeros((64, 64), F32)
        for k in range(XS):
            expert = (4 * (z * XS + k) + quarter).astype(F32)
            match = (meta == expert) & (lane < 8)
            here = col // 16 == k
            hit = jnp.where(here, jnp.sum(jnp.where(match, 1.0, 0.0), 1, keepdims=True), hit)
            whi = jnp.where(here, jnp.sum(jnp.where(match, high, 0.0), 1, keepdims=True), whi)
            wlo = jnp.where(here, jnp.sum(jnp.where(match, low, 0.0), 1, keepdims=True), wlo)
        before = jnp.dot(earlier, hit.astype(BF), preferred_element_type=F32)
        place = (2 * (tok // 8)).astype(F32) + before
        pick = jnp.where((col % 16).astype(F32) == place, hit, 0.0)
        chi[s] = (pick * whi).astype(BF)
        clo[s] = (pick * wlo).astype(BF)
        pick = pick.astype(BF)
        for lo, hi in CUTS:
            got_rows = lax.dot_general(
                pick, toks[s, :, lo:hi], (((0,), (0,)), ((), ())), preferred_element_type=F32
            )
            chosen[s, :, :, lo:hi] = got_rows.astype(BF).reshape(XS, 16, hi - lo)

    def ffn(s):
        block = rows[s].reshape(64, W)
        rest = mrows[s].reshape(64, EX)
        for n in range(3):
            cols = slice(n * 256, (n + 1) * 256)
            gate = jnp.dot(block, wg[:W, cols], preferred_element_type=F32) + jnp.dot(
                rest, wg[W:, cols], preferred_element_type=F32
            )
            lift = jnp.dot(block, wu[:W, cols], preferred_element_type=F32) + jnp.dot(
                rest, wu[W:, cols], preferred_element_type=F32
            )
            act[:, cols] = (gate / (1.0 + jnp.exp(-gate)) * lift).astype(BF)
        made = jnp.dot(act[...], wd[:, W:], preferred_element_type=F32)
        mouts[s] = made.astype(BF).reshape(XS, 16, EX)
        push(mouts.at[s], madd.at[s], nsend.at[s], nrecv.at[s], attn=mate)
        for lo, hi in CUTS:
            made = jnp.dot(act[...], wd[:, lo:hi], preferred_element_type=F32)
            fine[s, :, lo:hi] = made

    def spread(s, src, dst, ss, rr):
        for d in (2, 1, 3):
            push(
                src.at[s, xs[d]], dst.at[s, x], ss.at[s, d - 1], rr.at[s, x],
                expert=z * XS + xs[d],
            )

    def gathered(s, buf, rr):
        for d in (1, 3, 2):
            got(buf.at[s, xs[d]], rr.at[s, xs[d]])

    for n in range(RING + 6):
        if n < RING:
            s = SLOTS[n]
            if s:
                for h in range(2):
                    got(half(toks, s, h), trecv.at[s, h])
                    if s < 3 or (s == 3 and h == 0):
                        push(
                            half(toks, s, h), half(toks, s + 1, h), tsend.at[s, h, 0],
                            trecv.at[s + 1, h], expert=up,
                        )
                    if s > 5 or (s == 5 and h == 1):
                        push(
                            half(toks, s, h), half(toks, s - 1, h), tsend.at[s, h, 1],
                            trecv.at[s - 1, h], expert=down,
                        )
            choose(s)
            spread(s, chosen, rows, dsend, drecv)
            rows[s, pl.ds(x, 1)] = chosen[s, pl.ds(x, 1)]
        if 2 <= n < RING + 2:
            s = SLOTS[n - 2]
            gathered(s, rows, drecv)
            push(rows.at[s, :, :, shared], mrows.at[s], msend.at[s], mrecv.at[s], attn=mate)
        if 4 <= n < RING + 4:
            s = SLOTS[n - 4]
            got(mrows.at[s], mrecv.at[s])
            if n == 4:
                for load in loads:
                    load.wait()
            ffn(s)
        if 6 <= n:
            s = SLOTS[n - 6]
            got(madd.at[s], nrecv.at[s])
            fine[s, :, shared] = fine[s, :, shared] + madd[s].reshape(64, EX).astype(F32)
            outs[s] = fine[s].astype(BF).reshape(XS, 16, W)
            spread(s, outs, back, bsend, brecv)
            back[s, pl.ds(x, 1)] = outs[s, pl.ds(x, 1)]

    def combine(s, h):
        part = slice(32 * h, 32 * h + 32)
        made = back[s].reshape(64, W)
        return jnp.dot(chi[s, part, :], made, preferred_element_type=F32) + jnp.dot(
            clo[s, part, :], made, preferred_element_type=F32
        )

    for s in reversed(SLOTS):
        gathered(s, back, brecv)
        for h in range(2):
            value = combine(s, h)
            part = slice(32 * h, 32 * h + 32)
            if s == 0:
                for way in range(2):
                    got(zlast.at[way, pl.ds(32 * h, 32)], zfin.at[way, h])
                    value = value + zlast[way, part, :].astype(F32)
                for j in range(4):
                    row = 4 * h + j
                    ysum[row] = value[8 * j : 8 * j + 8].astype(BF)
                continue
            if s in (1, 2, 6, 7) or (s == 3 and h == 0) or (s == 5 and h == 1):
                got(half(zgot, s, h), zrecv.at[s, h])
                value = value + zgot[s, part, :].astype(F32)
            zsum[s, part, :] = value.astype(BF)
            downward = s < 4 or (s == 4 and h == 0)
            to = s - 1 if downward else (s + 1) % RING
            if to == 0:
                way = 0 if downward else 1
                push(
                    half(zsum, s, h), zlast.at[way, pl.ds(32 * h, 32)], zsend.at[s, h],
                    zfin.at[way, h], expert=down if downward else up,
                )
            else:
                push(
                    half(zsum, s, h), half(zgot, to, h), zsend.at[s, h], zrecv.at[to, h],
                    expert=down if downward else up,
                )
    for r in ORDER[:-1]:
        push(ysum.at[ys[r]], ygot.at[r], ysend.at[r], yrecv.at[r], attn=ys[r] * 2 + c)
    same = ysum[pl.ds(y, 1)].reshape(8, W).astype(F32)
    other = jnp.zeros((8, W), F32)
    for r in range(1, RING):
        got(ygot.at[r], yrecv.at[r])
        if r % 2 == 0:
            same = same + ygot[r].astype(F32)
        else:
            other = other + ygot[r].astype(F32)
    evens = jnp.where(odd == 0, same, other)
    odds = jnp.where(odd == 0, other, same)
    out_ref[:, :EX] = (stream_ref[:, :EX] + evens[:, :EX]).astype(BF)
    out_ref[:, EX:W] = (stream_ref[:, EX:W] + evens[:, EX:] + odds[:, : W - EX]).astype(BF)
    out_ref[:, W:] = (stream_ref[:, W:] + odds[:, W - EX :]).astype(BF)


def layer_kernel(
    lengths, q_ref, k_ref, v_ref, wo_ref, wg_ref, wu_ref, wd_ref, res_ref, gain_ref,
    ids_ref, gates_ref, out_ref,
    kbuf, vbuf, m_ref, l_ref, acc_ref, att_ref, send, recv,
    stream_ref, ht_ref, xin, part, zin, nbuf, gbuf, s1, s3, rx, rz, sy, ry,
    wg, wu, wd, wsem, wsend, wrecv, toks, *rest,
):
    a = lax.axis_index("attn")
    e = lax.axis_index("expert")
    y = a // 2
    c = a % 2
    odd = y % 2
    z = e // XS
    x = e % XS
    partner = y * 2 + (1 - c)
    own_cols = pl.ds(pl.multiple_of(odd * EX, 128), W)
    mate_cols = pl.ds(pl.multiple_of((1 - odd) * W, 128), EX)
    moves = []
    for n, (src, dst) in enumerate(((wg_ref.at[0], wg), (wu_ref.at[0], wu), (wd_ref.at[0], wd))):
        for i, (take, put) in enumerate(((own_cols, pl.ds(0, W)), (mate_cols, pl.ds(W, EX)))):
            for k in range(2):
                span = pl.ds(384 * k, 384)
                moves.append(
                    (2 * n + i, k, src.at[take], dst.at[put, span])
                    if n < 2
                    else (2 * n + i, k, src.at[:, take], dst.at[span, put])
                )
    loads = []
    for n, k, src, dst in moves:
        if k == 0:
            load = pltpu.make_async_copy(src, dst, wsem.at[n])
            load.start()
            loads.append(load)
    peers = [{"attn": partner}]
    peers += [{"attn": (y + r) % RING * 2 + c} for r in range(1, RING)]
    peers += [{"expert": (z + r) % RING * XS + x} for r in range(1, RING)]
    peers += [{"expert": z * XS + (x + d) % XS} for d in range(1, XS)]
    greet(peers)
    pending = []
    attention_stage(
        lengths, q_ref, k_ref, v_ref, att_ref, kbuf, vbuf, m_ref, l_ref, acc_ref, send, recv,
        pending,
    )
    for n, k, src, dst in moves:
        if k == 1:
            swap = remote(src, dst, wsend.at[n], wrecv.at[n], attn=partner)
            swap.start()
            loads.append(swap)
    mix_stage(
        att_ref, wo_ref, res_ref, gain_ref, ids_ref, gates_ref, stream_ref, toks,
        ht_ref, xin, part, zin, nbuf, gbuf, s1, s3, rx, rz, sy, ry, pending,
    )
    experts_stage(stream_ref, out_ref, wg, wu, wd, loads, toks, *rest, pending)
    for copy in pending:
        copy.wait_send()


def vmem(*shape, dtype=BF):
    return VM(shape, dtype)


def local(
    queries, keys, values, residual, prompt_lengths, out_proj, norm_gain,
    expert_ids, route_weights, w_gate, w_up, w_down,
):
    inv = pl.BlockSpec(memory_space=VM)
    anyw = pl.BlockSpec(memory_space=pl.ANY)
    smem = pl.BlockSpec(memory_space=pltpu.SMEM)
    return pl.pallas_call(
        layer_kernel,
        out_shape=jax.ShapeDtypeStruct((8, D), BF),
        in_specs=[smem, inv, inv, inv, inv, anyw, anyw, anyw, inv, inv, inv, inv],
        out_specs=inv,
        scratch_shapes=[
            vmem(16, 256, 128),
            vmem(16, 256, 128),
            vmem(256, 1, dtype=F32),
            vmem(256, 1, dtype=F32),
            vmem(256, 128, dtype=F32),
            vmem(256, 128),
            DMA((2, 8, 3)),
            DMA((2, 16)),
            vmem(8, D, dtype=F32),
            vmem(8, 4, 8, D),
            vmem(8, 3, 8, D),
            vmem(8, 8, D),
            vmem(8, 8, D),
            vmem(2, 8, TW),
            vmem(8, 8, TW),
            DMA((8, 3)),
            DMA((8,)),
            DMA((8, 3)),
            DMA((8,)),
            DMA((8,)),
            DMA((8,)),
            vmem(D, 768),
            vmem(D, 768),
            vmem(768, D),
            DMA((6,)),
            DMA((6,)),
            DMA((6,)),
            vmem(8, 64, TW),
            vmem(8, 4, 16, W),
            vmem(8, 4, 16, W),
            vmem(8, 4, 16, EX),
            vmem(64, 768),
            vmem(8, 4, 16, W),
            vmem(8, 4, 16, EX),
            vmem(8, 4, 16, EX),
            vmem(8, 64, W, dtype=F32),
            vmem(8, 4, 16, W),
            vmem(8, 64, 64),
            vmem(8, 64, 64),
            vmem(8, 64, W),
            vmem(8, 64, W),
            vmem(2, 64, W),
            vmem(8, 8, W),
            vmem(8, 8, W),
            DMA((8, 2, 2)),
            DMA((8, 2)),
            DMA((8, 3)),
            DMA((8, 4)),
            DMA((8,)),
            DMA((8,)),
            DMA((8,)),
            DMA((8,)),
            DMA((8, 3)),
            DMA((8, 4)),
            DMA((8, 2)),
            DMA((8, 2)),
            DMA((2, 2)),
            DMA((8,)),
            DMA((8,)),
        ],
        compiler_params=pltpu.CompilerParams(collective_id=0, has_side_effects=True),
        name="layer",
    )(
        prompt_lengths, queries, keys, values, out_proj, w_gate, w_up, w_down,
        residual, norm_gain.reshape(1, D), expert_ids, route_weights,
    )


def solution(mesh):
    return jax.shard_map(
        local,
        mesh=mesh,
        in_specs=(
            P("attn", "expert"),
            P(None, "attn", None),
            P(None, "attn", None),
            P(("attn", "expert"), None),
            P(),
            P("expert", None),
            P(),
            P(("attn", "expert"), None),
            P(("attn", "expert"), None),
            P("expert", None, "attn"),
            P("expert", None, "attn"),
            P("expert", "attn", None),
        ),
        out_specs=P(("attn", "expert"), None),
        check_vma=False,
    )
```
